256 devices in a mesh: dp: 8 (over z_lo, x), space: 32 (over z_hi, y, core).
Axes of the slice: x: 4, y: 4, z: 8 (z_hi: 4, z_lo: 2; z = z_hi * 2 + z_lo), core: 2. Of those that a mesh axis runs over, the one named last changes fastest.
Arguments:
- fields: bfloat16 [8, 128, 32, 32, 128], P('dp', 'space'), may hold values from -6 to 6
- cotangent: bfloat16 [8, 128, 32, 32, 128], P('dp', 'space'), may hold values from -6 to 6
- w_first: bfloat16 [3, 3, 128, 128], replicated, may hold values from -0.1875 to 0.1875
- w_second: bfloat16 [3, 3, 128, 128], replicated, may hold values from -0.1875 to 0.1875
- tile_links: int32 [128, 4, 5], P('space'), may hold values from 0 to 127, as said below
Outputs:
- mixed: bfloat16 [8, 128, 32, 32, 128], P('dp', 'space')
- grad_first: float32 [3, 3, 128, 128], replicated
- grad_second: float32 [3, 3, 128, 128], replicated
The draws below stay inside these ranges and needn't reach their ends.
Inputs may be any that keep to these rules, and one draw needn't show every extreme that they name: `tile_links`: columns 0 and 3 are tile numbers; columns 1 and 4 are an edge or corner 0 to 3; column 2 is 0 or 1. The links are mutual: if side k of tile t reads edge e of tile u with flag f, side e of u reads edge k of t with flag f; if corner k of t reads corner q of u, corner q of u reads corner k of t. Tiles 4 * d to 4 * d + 3 lie on index d of space; every source of a tile lies on its index, the next or the previous one, the last index being next to the first. Only the first 4 tiles of an index read from the previous index and only the last 4 from the next, each through exactly one side and the two corners at that side's ends; each tile read there is read through a side by exactly one tile of the reading index, and the corners read from it are the ends of that edge.
All inputs are finite; a program needn't handle non-finite values.
Results may differ from the reference program's by a relative error of at most 0.0031.
Values may be sent and summed in bfloat16 or wider, within the bound.
No kernel may reach another device: no remote copies, remote signals or barrier semaphores. Data moves between devices by JAX's collectives and lax.ppermute only.
A program may use at most 64 MiB of HBM per device.

```python
import jax
import jax.numpy as jnp
from jax import lax

C = 128
S = 32
BAND = 4
TILES = 128
SAMPLES = 8


def draw_tile_links(key, part):
    rotation = jax.random.randint(jax.random.fold_in(key, 11), (TILES,), 0, 4).astype(jnp.int32)
    tile_ids = jnp.arange(TILES, dtype=jnp.int32)
    line_count = TILES // BAND
    line_of = tile_ids // BAND
    column_of = tile_ids % BAND
    quarter = jnp.arange(4, dtype=jnp.int32)
    layout = (quarter[None, :] - rotation[:, None]) % 4
    side_line = jnp.where(layout == 0, -1, jnp.where(layout == 2, 1, 0))
    side_column = jnp.where(layout == 1, 1, jnp.where(layout == 3, -1, 0))
    side_source = (line_of[:, None] + side_line) % line_count * BAND + (column_of[:, None] + side_column) % BAND
    side_edge = ((layout + 2) % 4 + rotation[side_source]) % 4
    side_rev = ((quarter[None, :] < 2) == (side_edge < 2)).astype(jnp.int32)
    corner_line = jnp.where(layout < 2, -1, 1)
    corner_column = jnp.where((layout == 0) | (layout == 3), -1, 1)
    corner_source = (line_of[:, None] + corner_line) % line_count * BAND + (column_of[:, None] + corner_column) % BAND
    corner_at = ((layout + 2) % 4 + rotation[corner_source]) % 4
    return jnp.stack([side_source, side_edge, side_rev, corner_source, corner_at], axis=-1).astype(jnp.int32)


def block_scale(rng, shape, pieces, low, largest):
    def one(position, blocks):
        draws = jax.random.uniform(jax.random.fold_in(jax.random.fold_in(rng, 6), position), (blocks,), jnp.float32, low / len(pieces), largest / len(pieces))
        return jnp.repeat(jnp.exp(draws), shape[position] // blocks).reshape((-1,) + (1,) * (len(shape) - position - 1))

    level = one(*pieces[0])
    for cut in pieces[1:]:
        level = level * one(*cut)
    return level


def bell_draw(own_key, dims, scale, reach, shards=(), held_as=jnp.bfloat16):
    factor_of = block_scale(own_key, dims, shards, -0.22, 0.18) if shards else 1.0
    values = jax.random.normal(own_key, dims, jnp.float32) * scale * factor_of
    return jnp.minimum(jnp.maximum(values, -reach), reach).astype(held_as)


def setup_inputs(seed: int = 0) -> dict:
    keys = jax.random.split(jax.random.key(seed), 6)
    fields = bell_draw(keys[0], (SAMPLES, TILES, S, S, C), 1.0, 6.0, ((0, 8), (1, 32)))
    cotangent = bell_draw(keys[1], (SAMPLES, TILES, S, S, C), 1.0, 6.0, ((0, 8), (1, 32)))
    w_first = bell_draw(keys[2], (3, 3, C, C), (9 * C) ** -0.5, 0.1875)
    w_second = bell_draw(keys[3], (3, 3, C, C), (9 * C) ** -0.5, 0.1875)
    tile_links = draw_tile_links(jax.random.fold_in(keys[5], 71), 0)
    return dict(fields=fields, cotangent=cotangent, w_first=w_first, w_second=w_second, tile_links=tile_links)


def edge_strips(values_in):
    extent = values_in.shape[-2]
    top_row = values_in[..., 0, :, :]
    right_col = values_in[..., :, extent - 1, :]
    bottom_row = values_in[..., extent - 1, :, :]
    left_col = values_in[..., :, 0, :]
    sides = jnp.stack([top_row, right_col, bottom_row, left_col], axis=-3)
    corner_pix = jnp.stack([values_in[..., 0, 0, :], values_in[..., 0, extent - 1, :], values_in[..., extent - 1, extent - 1, :], values_in[..., extent - 1, 0, :]], axis=-2)
    return jnp.concatenate([sides, corner_pix[..., None, :]], axis=-2)

def assemble(values_in, pool_rows, side_rows, side_flip, corner_rows):
    extent = values_in.shape[-2]
    picked = pool_rows[side_rows]
    ghosts = picked[:, :, :extent, :]
    ghosts = jnp.where(side_flip[:, :, None, None] == 1, ghosts[:, :, ::-1, :], ghosts)
    corner_pix = pool_rows[corner_rows][:, :, extent, :]
    middle = jnp.concatenate([ghosts[:, 3, :, None, :], values_in, ghosts[:, 1, :, None, :]], axis=2)
    top_line = jnp.concatenate([corner_pix[:, 0:1], ghosts[:, 0], corner_pix[:, 1:2]], axis=1)
    bottom_line = jnp.concatenate([corner_pix[:, 3:4], ghosts[:, 2], corner_pix[:, 2:3]], axis=1)
    return jnp.concatenate([top_line[:, None], middle, bottom_line[:, None]], axis=1)

def ghost_grads(padded_grad, side_flip):
    sides = jnp.stack([padded_grad[:, 0, 1:-1], padded_grad[:, 1:-1, -1], padded_grad[:, -1, 1:-1], padded_grad[:, 1:-1, 0]], axis=1)
    sides = jnp.where(side_flip[:, :, None, None] == 1, sides[:, :, ::-1, :], sides)
    corner_pix = jnp.stack([padded_grad[:, 0, 0], padded_grad[:, 0, -1], padded_grad[:, -1, -1], padded_grad[:, -1, 0]], axis=1)
    return (sides, corner_pix)

def add_edges(gradient, returned):
    extent = gradient.shape[1]
    gradient = gradient.at[:, 0, :, :].add(returned[:, 0, :extent])
    gradient = gradient.at[:, :, extent - 1, :].add(returned[:, 1, :extent])
    gradient = gradient.at[:, extent - 1, :, :].add(returned[:, 2, :extent])
    gradient = gradient.at[:, :, 0, :].add(returned[:, 3, :extent])
    gradient = gradient.at[:, 0, 0, :].add(returned[:, 0, extent])
    gradient = gradient.at[:, 0, extent - 1, :].add(returned[:, 1, extent])
    gradient = gradient.at[:, extent - 1, extent - 1, :].add(returned[:, 2, extent])
    gradient = gradient.at[:, extent - 1, 0, :].add(returned[:, 3, extent])
    return gradient

def conv_valid(padded, kernel):
    return lax.conv_general_dilated(padded, kernel, (1, 1), 'VALID', dimension_numbers=('NHWC', 'HWIO', 'NHWC'), preferred_element_type=jnp.float32)

def conv_back(cotan, kernel):
    flipped = jnp.transpose(kernel[::-1, ::-1], (0, 1, 3, 2))
    return lax.conv_general_dilated(cotan, flipped, (1, 1), ((2, 2), (2, 2)), dimension_numbers=('NHWC', 'HWIO', 'NHWC'), preferred_element_type=jnp.float32)

def kernel_grad(padded, cotan):
    extent = cotan.shape[1]
    width = cotan.shape[-1]
    flat_cot = cotan.reshape(-1, width)
    blocks = []
    for row_off in range(3):
        for col_off in range(3):
            window = padded[:, row_off:row_off + extent, col_off:col_off + extent, :].reshape(-1, width)
            blocks.append(lax.dot_general(window, flat_cot, (((0,), (0,)), ((), ())), preferred_element_type=jnp.float32))
    return jnp.stack(blocks).reshape(3, 3, width, width)

def reference(fields, cotangent, w_first, w_second, tile_links):
    side_rows = (tile_links[:, :, 0] * 4 + tile_links[:, :, 1]).astype(jnp.int32)
    side_flip = tile_links[:, :, 2]
    corner_rows = (tile_links[:, :, 3] * 4 + tile_links[:, :, 4]).astype(jnp.int32)

    def one_sample(pair):
        sample_in, cotan = pair
        pool_in = edge_strips(sample_in).reshape(TILES * 4, S + 1, C)
        padded_in = assemble(sample_in, pool_in, side_rows, side_flip, corner_rows)
        hidden = conv_valid(padded_in, w_first)
        gate = jax.nn.sigmoid(hidden)
        active = (hidden * gate).astype(jnp.bfloat16)
        pool_act = edge_strips(active).reshape(TILES * 4, S + 1, C)
        padded_act = assemble(active, pool_act, side_rows, side_flip, corner_rows)
        mixed = (sample_in.astype(jnp.float32) + conv_valid(padded_act, w_second)).astype(jnp.bfloat16)
        grad_second = kernel_grad(padded_act, cotan)
        padded_grad = conv_back(cotan, w_second)
        sides, corner_pix = ghost_grads(padded_grad, side_flip)
        pool_sides = jnp.zeros((TILES * 4, S, C), jnp.float32).at[side_rows.reshape(-1)].add(sides.reshape(-1, S, C))
        pool_corner = jnp.zeros((TILES * 4, C), jnp.float32).at[corner_rows.reshape(-1)].add(corner_pix.reshape(-1, C))
        returned = jnp.concatenate([pool_sides, pool_corner[:, None]], axis=1).reshape(TILES, 4, S + 1, C)
        active_grad = add_edges(padded_grad[:, 1:-1, 1:-1], returned)
        hidden_grad = (active_grad * gate * (1.0 + hidden * (1.0 - gate))).astype(jnp.bfloat16)
        grad_first = kernel_grad(padded_in, hidden_grad)
        return (mixed, grad_first, grad_second)
    mixed, grad_first, grad_second = lax.map(one_sample, (fields, cotangent))
    scale = float(SAMPLES * TILES * S * S) ** (-0.5)
    return (mixed, lax.optimization_barrier(jnp.sum(grad_first, axis=0)) * scale, lax.optimization_barrier(jnp.sum(grad_second, axis=0)) * scale)
```

```python
import jax
import jax.numpy as jnp
from jax import lax
from jax.experimental import pallas as pl
from jax.experimental.pallas import tpu as pltpu
from jax.sharding import PartitionSpec as P

f32 = jnp.float32
bf16 = jnp.bfloat16
S = 32
C = 128
T = 4
PIX = S * S
GAP = 48
LEAD = 8
PAD = (S + 2) * GAP
WIDE = (S + 2) * S
RIM = 48
SEND = S + RIM
MESH = ("dp", "space")


def vmem():
    return pl.BlockSpec(memory_space=pltpu.VMEM)


def smem():
    return pl.BlockSpec(memory_space=pltpu.SMEM)


def call(body, outs, ins, scratch=(), smem_outs=(), limit=40):
    return pl.pallas_call(
        body,
        out_shape=outs,
        in_specs=[smem() if k == "s" else vmem() for k in ins],
        out_specs=[smem() if i in smem_outs else vmem() for i in range(len(outs))],
        scratch_shapes=list(scratch),
        compiler_params=pltpu.CompilerParams(vmem_limit_bytes=limit << 20),
    )


def shape(dims, dtype):
    return jax.ShapeDtypeStruct(dims, dtype)


def flip8(block):
    row = lax.broadcasted_iota(jnp.int32, (8, C), 0)
    block = pltpu.roll(block, 4, 0)
    block = jnp.where((row & 2) == 0, pltpu.roll(block, 6, 0), pltpu.roll(block, 2, 0))
    return jnp.where((row & 1) == 0, pltpu.roll(block, 7, 0), pltpu.roll(block, 1, 0))


def flip_line(line):
    parts = [line[8 * i : 8 * i + 8] for i in range(S // 8)]
    return jnp.concatenate([flip8(part) for part in reversed(parts)], axis=0)


def directed(line, flag):
    return jnp.where(jnp.full(line.shape, flag, jnp.int32) == 1, flip_line(line), line)


def link_table(own, links, table, count):
    zero = jnp.int32(0)

    def where_is(source):
        gap = (source >> 2) - own + 1
        gap = jnp.where(gap < 0, gap + count, gap)
        return jnp.where(gap >= count, gap - count, gap), source & 3

    sides = []
    facing = {(way, slot): zero for way in (0, 2) for slot in range(T)}
    for n in range(4 * T):
        rel, slot = where_is(links[n, 0])
        edge = links[n, 1]
        sides.append((rel, slot, edge))
        for way in (0, 2):
            for s in range(T):
                facing[way, s] += jnp.where((rel == way) & (slot == s), edge, zero)
    for n, (rel, slot, edge) in enumerate(sides):
        line = jnp.where(rel == 1, slot * 4 + edge, jnp.where(rel == 0, 16 + slot, 20 + slot))
        table[n, 0] = line
        table[n, 1] = links[n, 2]
    for n in range(4 * T):
        rel, slot = where_is(links[n, 3])
        at = links[n, 4]
        low, high = zero, zero
        for s in range(T):
            low += jnp.where(slot == s, facing[0, s], zero)
            high += jnp.where(slot == s, facing[2, s], zero)
        face = jnp.where(rel == 0, low, high)
        start = jnp.where(face == 1, 1, jnp.where(face == 2, 3, 0))
        near = slot * 4 + jnp.where(at < 2, 0, 2)
        line = jnp.where(rel == 1, near, jnp.where(rel == 0, 16 + slot, 20 + slot))
        far_end = jnp.where(at == start, 0, 1)
        near_end = jnp.where((at == 1) | (at == 2), 1, 0)
        table[16 + n, 0] = line
        table[16 + n, 1] = jnp.where(rel == 1, near_end, far_end)
    faces = []
    for t in range(T):
        low, high = zero, zero
        for k in range(4):
            rel = sides[t * 4 + k][0]
            low += jnp.where(rel == 0, k, 0)
            high += jnp.where(rel == 2, k, 0)
        table[32 + t, 0] = low
        table[32 + t, 1] = high
        faces.append((low, high))
    return faces


def make_edges_body(count):
    def body(own, links, fields, cot, w_second, table, low, high, rim, lines, wide, slab):
        faces = link_table(own[0], links, table, count)

        def put_lines(source, t, store):
            store(0, source[t, 0].astype(f32))
            store(2, source[t, S - 1].astype(f32))
            for edge, first, at in ((3, 0, 0), (1, 16, 15)):
                slab[...] = source[t, :, first : first + 16, :].astype(f32).reshape(16 * S, C)
                store(edge, slab[pl.ds(at, S, stride=16), :])

        for t in range(T):

            def store(k, line, t=t):
                lines[(t * 4 + k) * S : (t * 4 + k + 1) * S, :] = line

            put_lines(fields, t, store)
        wide[...] = jnp.zeros(wide.shape, f32)
        for t in range(T):

            def store(k, line, t=t):
                wide[(k * T + t) * 64 + 16 : (k * T + t) * 64 + 16 + S, :] = line

            put_lines(cot, t, store)
        taps = {
            0: [(0, c) for c in range(3)],
            1: [(r, 2) for r in range(3)],
            2: [(2, c) for c in range(3)],
            3: [(r, 0) for r in range(3)],
        }
        for k in range(4):
            left = []
            for t in range(T):
                base = (k * T + t) * 64
                left.append(
                    jnp.concatenate(
                        [wide[base + 9 - c : base + 9 - c + RIM, :].astype(bf16) for c in range(3)],
                        axis=1,
                    )
                )
            left = jnp.concatenate(left, axis=0)
            right = jnp.concatenate([w_second[r, c] for r, c in taps[k]], axis=1)
            out = lax.dot_general(
                left, right, (((1,), (1,)), ((), ())), preferred_element_type=f32
            )
            for t in range(T):
                rim[(t * 4 + k) * RIM : (t * 4 + k + 1) * RIM, :] = out[t * RIM : (t + 1) * RIM]
        for t in range(T):
            for out_ref, face in zip((low, high), faces[t]):
                n = t * 4 + face
                at = pl.multiple_of(n * S, S)
                out_ref[t, 0:S, :] = lines[pl.ds(at, S), :].astype(bf16)
                at = pl.multiple_of(n * RIM, 16)
                out_ref[t, S:SEND, :] = rim[pl.ds(at, RIM), :].astype(bf16)

    return body


def widen(padded, t, wide):
    for p in range(S + 2):
        for c in range(3):
            at = p * GAP + LEAD - 1 + c
            wide[t, p * S : (p + 1) * S, c * C : (c + 1) * C] = padded[t, at : at + S, :].astype(bf16)


def taps_of(wide, t, first, rows):
    return jnp.concatenate(
        [wide[t, r * S + first : r * S + first + rows, :] for r in range(3)], axis=1
    )


def put_interior(source, padded, t):
    for r in range(S):
        at = (1 + r) * GAP + LEAD
        padded[t, at : at + S, :] = source[t, r].astype(f32)


def conv_back_body(cot, w_second, out, padded, wide):
    right = jnp.concatenate(
        [w_second[2 - r, 2 - c] for r in range(3) for c in range(3)], axis=1
    )

    def one(t, carry):
        zero = jnp.zeros((GAP, C), f32)
        padded[t, 0:GAP, :] = zero
        padded[t, PAD - GAP : PAD, :] = zero
        for r in range(S):
            at = (1 + r) * GAP
            padded[t, at : at + 8, :] = zero[:8]
            padded[t, at + LEAD + S : at + GAP, :] = zero[:8]
        put_interior(cot, padded, t)
        widen(padded, t, wide)
        for first in range(0, PIX, 256):
            out[t, first : first + 256, :] = lax.dot_general(
                taps_of(wide, t, first, 256),
                right,
                (((1,), (1,)), ((), ())),
                preferred_element_type=f32,
            )
        return carry

    lax.fori_loop(0, T, one, 0)


def collect_lines(padded, lines, low, high):
    for t in range(T):
        base = GAP + LEAD
        spots = {
            0: padded[t, base : base + S, :],
            1: padded[t, pl.ds(base + S - 1, S, stride=GAP), :],
            2: padded[t, base + (S - 1) * GAP : base + (S - 1) * GAP + S, :],
            3: padded[t, pl.ds(base, S, stride=GAP), :],
        }
        for k in range(4):
            lines[(t * 4 + k) * S : (t * 4 + k + 1) * S, :] = spots[k]
        for first, received in ((16, low), (20, high)):
            lines[(first + t) * S : (first + t + 1) * S, :] = received[t, 0:S, :].astype(f32)


def put_rims(table, lines, padded):
    for t in range(T):
        for k in range(4):
            n = t * 4 + k
            at = pl.multiple_of(table[n, 0] * S, S)
            line = directed(lines[pl.ds(at, S), :], table[n, 1])
            if k == 0:
                padded[t, LEAD : LEAD + S, :] = line
            elif k == 2:
                at = (S + 1) * GAP + LEAD
                padded[t, at : at + S, :] = line
            elif k == 1:
                padded[t, pl.ds(GAP + LEAD + S, S, stride=GAP), :] = line
            else:
                padded[t, pl.ds(GAP + LEAD - 1, S, stride=GAP), :] = line
        for k, spot in enumerate(
            (
                LEAD - 1,
                LEAD + S,
                (S + 1) * GAP + LEAD + S,
                (S + 1) * GAP + LEAD - 1,
            )
        ):
            n = 16 + t * 4 + k
            at = table[n, 0] * S + table[n, 1] * (S - 1)
            padded[t, spot : spot + 1, :] = lines[pl.ds(at, 1), :]


def forward_body(
    table, fields, low, high, rim, interior, w_first,
    active, hidden_grad, wide, send_low, send_high,
    padded, lines, rims, grads, rounded, edges,
):
    for t in range(T):
        put_interior(fields, padded, t)
    collect_lines(padded, lines, low, high)
    put_rims(table, lines, padded)
    rims[0 : 16 * RIM, :] = rim[...]
    for t in range(T):
        rims[(16 + t) * RIM : (17 + t) * RIM, :] = low[t, S:SEND, :].astype(f32)
        rims[(20 + t) * RIM : (21 + t) * RIM, :] = high[t, S:SEND, :].astype(f32)
    for t in range(T):
        grads[t] = interior[t]
        for k in range(4):
            n = t * 4 + k
            at = pl.multiple_of(table[n, 0] * RIM, 16)
            line = directed(rims[pl.ds(at + 8, S), :], table[n, 1])
            if k == 0:
                grads[t, 0:S, :] += line
            elif k == 2:
                grads[t, PIX - S : PIX, :] += line
            else:
                spot = pl.ds(S - 1 if k == 1 else 0, S, stride=S)
                grads[t, spot, :] = grads[t, spot, :] + line
        for k, spot in enumerate((0, S - 1, PIX - 1, PIX - S)):
            n = 16 + t * 4 + k
            at = table[n, 0] * RIM + 7 + table[n, 1] * (S + 1)
            grads[t, spot : spot + 1, :] += rims[pl.ds(at, 1), :]
    right = jnp.concatenate([w_first[r, c] for r in range(3) for c in range(3)], axis=0)

    def one(t, carry):
        widen(padded, t, wide)
        for first in range(0, PIX, 256):
            hidden = jnp.dot(taps_of(wide, t, first, 256), right, preferred_element_type=f32)
            gate = 1.0 / (1.0 + jnp.exp(-hidden))
            act = (hidden * gate).astype(bf16)
            active[t, first // S : first // S + 8] = act.reshape(8, S, C)
            rounded[first : first + 256, :] = act.astype(f32)
            back = grads[t, first : first + 256, :]
            hidden_grad[t, first : first + 256, :] = (
                back * gate * (1.0 + hidden * (1.0 - gate))
            ).astype(bf16)
        edges[0:S, :] = rounded[0:S, :]
        edges[S : 2 * S, :] = rounded[pl.ds(S - 1, S, stride=S), :]
        edges[2 * S : 3 * S, :] = rounded[PIX - S : PIX, :]
        edges[3 * S : 4 * S, :] = rounded[pl.ds(0, S, stride=S), :]
        for out_ref, which in ((send_low, 0), (send_high, 1)):
            at = pl.multiple_of(table[32 + t, which] * S, S)
            out_ref[t] = edges[pl.ds(at, S), :].astype(bf16)
        return carry

    lax.fori_loop(0, T, one, 0)


def weight_grad(cot_of, wide, acc, out):
    acc[...] = jnp.zeros(acc.shape, f32)

    def one(t, carry):
        left = cot_of(t).T
        for r in range(3):
            acc[:, r * 3 * C : (r + 1) * 3 * C] += jnp.dot(
                left, wide[t, r * S : r * S + PIX, :], preferred_element_type=f32
            )
        return carry

    lax.fori_loop(0, T, one, 0)
    for n in range(9):
        out[n * C : (n + 1) * C, :] = acc[:, n * C : (n + 1) * C].T


def first_grad_body(hidden_grad, wide, out, acc):
    weight_grad(lambda t: hidden_grad[t], wide, acc, out)


def second_grad_body(table, active, low, high, cot, out, wide, padded, lines, acc):
    for t in range(T):
        put_interior(active, padded, t)
    collect_lines(padded, lines, low, high)
    put_rims(table, lines, padded)

    def one(t, carry):
        widen(padded, t, wide)
        return carry

    lax.fori_loop(0, T, one, 0)
    weight_grad(lambda t: cot[t].reshape(PIX, C), wide, acc, out)


def mixed_body(fields, wide, w_second, out):
    right = jnp.concatenate([w_second[r, c] for r in range(3) for c in range(3)], axis=0)

    def one(t, carry):
        for first in range(0, PIX, 256):
            got = jnp.dot(taps_of(wide, t, first, 256), right, preferred_element_type=f32)
            rows = slice(first // S, first // S + 8)
            out[t, rows] = (
                fields[t, rows].astype(f32) + got.reshape(8, S, C)
            ).astype(bf16)
        return carry

    lax.fori_loop(0, T, one, 0)


def place_of(index):
    dp, space = divmod(index, 32)
    z_low, x = divmod(dp, 4)
    z_high, rest = divmod(space, 8)
    y, core = divmod(rest, 2)
    return dict(x=x, y=y, z=z_high * 2 + z_low, core=core)


def index_of(place):
    z_high, z_low = divmod(place["z"], 2)
    return (z_low * 4 + place["x"]) * 32 + z_high * 8 + place["y"] * 2 + place["core"]


def exchange(value, moves):
    pairs = []
    for index in range(256):
        place = place_of(index)
        axis, mask = moves[place["core"]]
        place[axis] ^= mask
        pairs.append((index, index_of(place)))
    return lax.ppermute(value, MESH, pairs)


def halve(value, moves, bit, dtype):
    rows = value.shape[0] // 2
    low, high = value[:rows], value[rows:]
    sent = exchange(jnp.where(bit == 0, high, low).astype(dtype), moves)
    return jnp.where(bit == 0, low, high) + sent.astype(f32)


def double(value, moves):
    return value + exchange(value, moves)


def join(value, moves, bit):
    other = exchange(value, moves)
    return jnp.where(
        bit == 0, jnp.concatenate([value, other]), jnp.concatenate([other, value])
    )


def sum_everywhere(first, second, scale):
    dp, space = lax.axis_index("dp"), lax.axis_index("space")
    core = space % 2
    x, y = dp % 4, (space // 2) % 4
    gray_x, gray_y = (x ^ (x >> 1)) & 1, (y ^ (y >> 1)) & 1
    swap = (("core", 1), ("core", 1))
    step1, bit1 = (("x", 1), ("y", 1)), jnp.where(core == 0, gray_x, gray_y)
    step2, bit2 = (("y", 1), ("x", 1)), jnp.where(core == 0, gray_y, gray_x)
    step3, bit3 = (("x", 3), ("y", 3)), jnp.where(core == 0, x >> 1, y >> 1)
    sent = exchange(jnp.where(core == 0, second, first), swap)
    value = jnp.where(core == 0, first, second) + sent
    value = halve(value, step1, bit1, bf16)
    value = halve(value, step2, bit2, bf16)
    value = halve(value, step3, bit3, f32)
    value = double(value, (("y", 3), ("z", 1)))
    value = double(value, (("z", 1), ("x", 3)))
    value = double(value, (("z", 2), ("z", 2)))
    value = double(value, (("z", 7), ("z", 7)))
    value = (value * scale).astype(bf16)
    value = join(value, step3, bit3)
    value = join(value, step2, bit2)
    value = join(value, step1, bit1)
    other = exchange(value, swap)
    return (
        jnp.where(core == 0, value, other).astype(f32),
        jnp.where(core == 0, other, value).astype(f32),
    )


def local(fields, cotangent, w_first, w_second, tile_links):
    count = lax.axis_size("space")
    own = lax.axis_index("space").astype(jnp.int32).reshape(1)
    links = tile_links.reshape(4 * T, 5)
    x = fields.reshape(T, S, S, C)
    cot = cotangent.reshape(T, S, S, C)
    up = [(i, (i + 1) % count) for i in range(count)]
    down = [(j, i) for i, j in up]
    table, low, high, rim = call(
        make_edges_body(count),
        [
            shape((36, 2), jnp.int32),
            shape((T, SEND, C), bf16),
            shape((T, SEND, C), bf16),
            shape((16 * RIM, C), f32),
        ],
        "ssvvv",
        [
            pltpu.VMEM((16 * S, C), f32),
            pltpu.VMEM((16 * 64, C), f32),
            pltpu.VMEM((16 * S, C), f32),
        ],
        smem_outs=(0,),
    )(own, links, x, cot, w_second)
    from_low = lax.ppermute(high, "space", up)
    from_high = lax.ppermute(low, "space", down)
    (interior,) = call(
        conv_back_body,
        [shape((T, PIX, C), f32)],
        "vv",
        [pltpu.VMEM((T, PAD, C), f32), pltpu.VMEM((T, WIDE, 3 * C), bf16)],
    )(cot, w_second)
    active, hidden_grad, wide, act_low, act_high = call(
        forward_body,
        [
            shape((T, S, S, C), bf16),
            shape((T, PIX, C), bf16),
            shape((T, WIDE, 3 * C), bf16),
            shape((T, S, C), bf16),
            shape((T, S, C), bf16),
        ],
        "svvvvvv",
        [
            pltpu.VMEM((T, PAD, C), f32),
            pltpu.VMEM((24 * S, C), f32),
            pltpu.VMEM((24 * RIM, C), f32),
            pltpu.VMEM((T, PIX, C), f32),
            pltpu.VMEM((PIX, C), f32),
            pltpu.VMEM((4 * S, C), f32),
        ],
    )(table, x, from_low, from_high, rim, interior, w_first)
    act_from_low = lax.ppermute(act_high, "space", up)
    act_from_high = lax.ppermute(act_low, "space", down)
    (grad_first,) = call(
        first_grad_body, [shape((9 * C, C), f32)], "vv", [pltpu.VMEM((C, 9 * C), f32)]
    )(hidden_grad, wide)
    grad_second, wide_active = call(
        second_grad_body,
        [shape((9 * C, C), f32), shape((T, WIDE, 3 * C), bf16)],
        "svvvv",
        [
            pltpu.VMEM((T, PAD, C), f32),
            pltpu.VMEM((24 * S, C), f32),
            pltpu.VMEM((C, 9 * C), f32),
        ],
    )(table, active, act_from_low, act_from_high, cot)
    (mixed,) = call(mixed_body, [shape((T, S, S, C), bf16)], "vvv")(x, wide_active, w_second)
    total = lax.axis_size("dp") * count * T * PIX
    first, second = sum_everywhere(grad_first, grad_second, float(total) ** -0.5)
    return (
        mixed.reshape(fields.shape),
        first.reshape(3, 3, C, C),
        second.reshape(3, 3, C, C),
    )


def solution(mesh):
    placed = (
        P("dp", "space", None, None, None),
        P("dp", "space", None, None, None),
        P(),
        P(),
        P("space", None, None),
    )
    return jax.shard_map(
        local,
        mesh=mesh,
        in_specs=placed,
        out_specs=(P("dp", "space", None, None, None), P(), P()),
        check_vma=False,
    )
```

```python
import jax
import jax.numpy as jnp
from jax import lax
from jax.experimental import pallas as pl
from jax.experimental.pallas import tpu as pltpu
from jax.sharding import PartitionSpec as P

f32 = jnp.float32
bf16 = jnp.bfloat16
S = 32
C = 128
T = 4
PIX = S * S
GAP = 48
LEAD = 8
PAD = (S + 2) * GAP
WIDE = (S + 2) * S
RIM = 48
SEND = S + RIM
MESH = ("dp", "space")


def vmem():
    return pl.BlockSpec(memory_space=pltpu.VMEM)


def smem():
    return pl.BlockSpec(memory_space=pltpu.SMEM)


def hbm():
    return pl.BlockSpec(memory_space=pltpu.HBM)


SPACES = {"s": smem, "v": vmem, "h": hbm}


def call(body, outs, ins, scratch=(), outs_in="", aliases={}, limit=16):
    return pl.pallas_call(
        body,
        out_shape=outs,
        in_specs=[SPACES[k]() for k in ins],
        out_specs=[SPACES[k]() for k in outs_in or "v" * len(outs)],
        scratch_shapes=list(scratch),
        input_output_aliases=aliases,
        compiler_params=pltpu.CompilerParams(vmem_limit_bytes=limit << 20),
    )


def shape(dims, dtype):
    return jax.ShapeDtypeStruct(dims, dtype)


def flip8(block):
    row = lax.broadcasted_iota(jnp.int32, (8, C), 0)
    block = pltpu.roll(block, 4, 0)
    block = jnp.where((row & 2) == 0, pltpu.roll(block, 6, 0), pltpu.roll(block, 2, 0))
    return jnp.where((row & 1) == 0, pltpu.roll(block, 7, 0), pltpu.roll(block, 1, 0))


def flip_line(line):
    parts = [line[8 * i : 8 * i + 8] for i in range(S // 8)]
    return jnp.concatenate([flip8(part) for part in reversed(parts)], axis=0)


def directed(line, flag):
    return jnp.where(jnp.full(line.shape, flag, jnp.int32) == 1, flip_line(line), line)


def link_table(own, links, table, count):
    zero = jnp.int32(0)

    def where_is(source):
        gap = (source >> 2) - own + 1
        gap = jnp.where(gap < 0, gap + count, gap)
        return jnp.where(gap >= count, gap - count, gap), source & 3

    sides = []
    facing = {(way, slot): zero for way in (0, 2) for slot in range(T)}
    for n in range(4 * T):
        rel, slot = where_is(links[n // 4, n % 4, 0])
        edge = links[n // 4, n % 4, 1]
        sides.append((rel, slot, edge))
        for way in (0, 2):
            for s in range(T):
                facing[way, s] += jnp.where((rel == way) & (slot == s), edge, zero)
    for n, (rel, slot, edge) in enumerate(sides):
        line = jnp.where(rel == 1, slot * 4 + edge, jnp.where(rel == 0, 16 + slot, 20 + slot))
        table[n, 0] = line
        table[n, 1] = links[n // 4, n % 4, 2]
    for n in range(4 * T):
        rel, slot = where_is(links[n // 4, n % 4, 3])
        at = links[n // 4, n % 4, 4]
        low, high = zero, zero
        for s in range(T):
            low += jnp.where(slot == s, facing[0, s], zero)
            high += jnp.where(slot == s, facing[2, s], zero)
        face = jnp.where(rel == 0, low, high)
        start = jnp.where(face == 1, 1, jnp.where(face == 2, 3, 0))
        near = slot * 4 + jnp.where(at < 2, 0, 2)
        line = jnp.where(rel == 1, near, jnp.where(rel == 0, 16 + slot, 20 + slot))
        far_end = jnp.where(at == start, 0, 1)
        near_end = jnp.where((at == 1) | (at == 2), 1, 0)
        table[16 + n, 0] = line
        table[16 + n, 1] = jnp.where(rel == 1, near_end, far_end)
    faces = []
    for t in range(T):
        low, high = zero, zero
        for k in range(4):
            rel = sides[t * 4 + k][0]
            low += jnp.where(rel == 0, k, 0)
            high += jnp.where(rel == 2, k, 0)
        table[32 + t, 0] = low
        table[32 + t, 1] = high
        faces.append((low, high))
    return faces


def make_edges_body(count):
    def body(
        own, tile_links, fields_far, cot_far, w_second_far,
        table, low, high, rim, fields, cot, w_second,
        lines, wide, slab, links, sems,
    ):
        copies = [
            pltpu.make_async_copy(source, target, sems.at[n])
            for n, (source, target) in enumerate(
                (
                    (tile_links, links),
                    (cot_far, cot),
                    (w_second_far, w_second),
                    (fields_far, fields),
                )
            )
        ]
        for copy in copies:
            copy.start()
        wide[...] = jnp.zeros(wide.shape, f32)
        copies[0].wait()
        faces = link_table(own[0], links, table, count)

        def put_lines(source, t, store):
            store(0, source[t, 0].astype(f32))
            store(2, source[t, S - 1].astype(f32))
            for edge, first, at in ((3, 0, 0), (1, 16, 15)):
                slab[...] = source[t, :, first : first + 16, :].astype(f32).reshape(16 * S, C)
                store(edge, slab[pl.ds(at, S, stride=16), :])

        copies[1].wait()
        for t in range(T):

            def store(k, line, t=t):
                wide[(k * T + t) * 64 + 16 : (k * T + t) * 64 + 16 + S, :] = line

            put_lines(cot, t, store)
        taps = {
            0: [(0, c) for c in range(3)],
            1: [(r, 2) for r in range(3)],
            2: [(2, c) for c in range(3)],
            3: [(r, 0) for r in range(3)],
        }
        copies[2].wait()
        for k in range(4):
            left = []
            for t in range(T):
                base = (k * T + t) * 64
                left.append(
                    jnp.concatenate(
                        [wide[base + 9 - c : base + 9 - c + RIM, :].astype(bf16) for c in range(3)],
                        axis=1,
                    )
                )
            left = jnp.concatenate(left, axis=0)
            right = jnp.concatenate([w_second[r, c] for r, c in taps[k]], axis=1)
            out = lax.dot_general(
                left, right, (((1,), (1,)), ((), ())), preferred_element_type=f32
            )
            for t in range(T):
                rim[(t * 4 + k) * RIM : (t * 4 + k + 1) * RIM, :] = out[t * RIM : (t + 1) * RIM]
        copies[3].wait()
        for t in range(T):

            def store(k, line, t=t):
                lines[(t * 4 + k) * S : (t * 4 + k + 1) * S, :] = line

            put_lines(fields, t, store)
        for t in range(T):
            for out_ref, face in zip((low, high), faces[t]):
                n = t * 4 + face
                at = pl.multiple_of(n * S, S)
                out_ref[t, 0:S, :] = lines[pl.ds(at, S), :].astype(bf16)
                at = pl.multiple_of(n * RIM, 16)
                out_ref[t, S:SEND, :] = rim[pl.ds(at, RIM), :].astype(bf16)

    return body


def widen(padded, t, wide):
    for p in range(S + 2):
        for c in range(3):
            at = p * GAP + LEAD - 1 + c
            wide[t, p * S : (p + 1) * S, c * C : (c + 1) * C] = padded[t, at : at + S, :].astype(bf16)


def taps_of(wide, t, first, rows):
    return jnp.concatenate(
        [wide[t, r * S + first : r * S + first + rows, :] for r in range(3)], axis=1
    )


def put_interior(source, padded, t):
    for r in range(S):
        at = (1 + r) * GAP + LEAD
        padded[t, at : at + S, :] = source[t, r].astype(f32)


def conv_back_body(cot, w_second, out, padded, wide):
    right = jnp.concatenate(
        [w_second[2 - r, 2 - c] for r in range(3) for c in range(3)], axis=1
    )

    def one(t, carry):
        zero = jnp.zeros((GAP, C), f32)
        padded[t, 0:GAP, :] = zero
        padded[t, PAD - GAP : PAD, :] = zero
        for r in range(S):
            at = (1 + r) * GAP
            padded[t, at : at + 8, :] = zero[:8]
            padded[t, at + LEAD + S : at + GAP, :] = zero[:8]
        put_interior(cot, padded, t)
        widen(padded, t, wide)
        for first in range(0, PIX, 256):
            out[t, first : first + 256, :] = lax.dot_general(
                taps_of(wide, t, first, 256),
                right,
                (((1,), (1,)), ((), ())),
                preferred_element_type=f32,
            )
        return carry

    lax.fori_loop(0, T, one, 0)


def collect_lines(padded, lines, low, high):
    for t in range(T):
        base = GAP + LEAD
        spots = {
            0: padded[t, base : base + S, :],
            1: padded[t, pl.ds(base + S - 1, S, stride=GAP), :],
            2: padded[t, base + (S - 1) * GAP : base + (S - 1) * GAP + S, :],
            3: padded[t, pl.ds(base, S, stride=GAP), :],
        }
        for k in range(4):
            lines[(t * 4 + k) * S : (t * 4 + k + 1) * S, :] = spots[k]
        for first, received in ((16, low), (20, high)):
            lines[(first + t) * S : (first + t + 1) * S, :] = received[t, 0:S, :].astype(f32)


def put_rims(table, lines, padded):
    for t in range(T):
        for k in range(4):
            n = t * 4 + k
            at = pl.multiple_of(table[n, 0] * S, S)
            line = directed(lines[pl.ds(at, S), :], table[n, 1])
            if k == 0:
                padded[t, LEAD : LEAD + S, :] = line
            elif k == 2:
                at = (S + 1) * GAP + LEAD
                padded[t, at : at + S, :] = line
            elif k == 1:
                padded[t, pl.ds(GAP + LEAD + S, S, stride=GAP), :] = line
            else:
                padded[t, pl.ds(GAP + LEAD - 1, S, stride=GAP), :] = line
        for k, spot in enumerate(
            (
                LEAD - 1,
                LEAD + S,
                (S + 1) * GAP + LEAD + S,
                (S + 1) * GAP + LEAD - 1,
            )
        ):
            n = 16 + t * 4 + k
            at = table[n, 0] * S + table[n, 1] * (S - 1)
            padded[t, spot : spot + 1, :] = lines[pl.ds(at, 1), :]


def forward_body(
    table, fields, low, high, rim, interior, w_first,
    active, hidden_grad, wide, send_low, send_high,
    padded, lines, rims, grads, rounded, edges,
):
    for t in range(T):
        put_interior(fields, padded, t)
    collect_lines(padded, lines, low, high)
    put_rims(table, lines, padded)
    rims[0 : 16 * RIM, :] = rim[...]
    for t in range(T):
        rims[(16 + t) * RIM : (17 + t) * RIM, :] = low[t, S:SEND, :].astype(f32)
        rims[(20 + t) * RIM : (21 + t) * RIM, :] = high[t, S:SEND, :].astype(f32)
    for t in range(T):
        grads[t] = interior[t]
        for k in range(4):
            n = t * 4 + k
            at = pl.multiple_of(table[n, 0] * RIM, 16)
            line = directed(rims[pl.ds(at + 8, S), :], table[n, 1])
            if k == 0:
                grads[t, 0:S, :] += line
            elif k == 2:
                grads[t, PIX - S : PIX, :] += line
            else:
                spot = pl.ds(S - 1 if k == 1 else 0, S, stride=S)
                grads[t, spot, :] = grads[t, spot, :] + line
        for k, spot in enumerate((0, S - 1, PIX - 1, PIX - S)):
            n = 16 + t * 4 + k
            at = table[n, 0] * RIM + 7 + table[n, 1] * (S + 1)
            grads[t, spot : spot + 1, :] += rims[pl.ds(at, 1), :]
    right = jnp.concatenate([w_first[r, c] for r in range(3) for c in range(3)], axis=0)

    def one(t, carry):
        widen(padded, t, wide)
        for first in range(0, PIX, 256):
            hidden = jnp.dot(taps_of(wide, t, first, 256), right, preferred_element_type=f32)
            gate = 1.0 / (1.0 + jnp.exp(-hidden))
            act = (hidden * gate).astype(bf16)
            active[t, first // S : first // S + 8] = act.reshape(8, S, C)
            rounded[first : first + 256, :] = act.astype(f32)
            back = grads[t, first : first + 256, :]
            hidden_grad[t, first : first + 256, :] = (
                back * gate * (1.0 + hidden * (1.0 - gate))
            ).astype(bf16)
        edges[0:S, :] = rounded[0:S, :]
        edges[S : 2 * S, :] = rounded[pl.ds(S - 1, S, stride=S), :]
        edges[2 * S : 3 * S, :] = rounded[PIX - S : PIX, :]
        edges[3 * S : 4 * S, :] = rounded[pl.ds(0, S, stride=S), :]
        for out_ref, which in ((send_low, 0), (send_high, 1)):
            at = pl.multiple_of(table[32 + t, which] * S, S)
            out_ref[t] = edges[pl.ds(at, S), :].astype(bf16)
        return carry

    lax.fori_loop(0, T, one, 0)


def weight_grad(cot_of, wide, acc, out):
    acc[...] = jnp.zeros(acc.shape, f32)

    def one(t, carry):
        left = cot_of(t).T
        for r in range(3):
            acc[:, r * 3 * C : (r + 1) * 3 * C] += jnp.dot(
                left, wide[t, r * S : r * S + PIX, :], preferred_element_type=f32
            )
        return carry

    lax.fori_loop(0, T, one, 0)
    for n in range(9):
        out[n * C : (n + 1) * C, :] = acc[:, n * C : (n + 1) * C].T


def first_grad_body(hidden_grad, wide, out, acc):
    weight_grad(lambda t: hidden_grad[t], wide, acc, out)


def second_grad_body(table, active, low, high, cot, out, wide, padded, lines, acc):
    for t in range(T):
        put_interior(active, padded, t)
    collect_lines(padded, lines, low, high)
    put_rims(table, lines, padded)

    def one(t, carry):
        widen(padded, t, wide)
        return carry

    lax.fori_loop(0, T, one, 0)
    weight_grad(lambda t: cot[t].reshape(PIX, C), wide, acc, out)


def make_mixed_body(begin, end):
    def body(fields, wide, w_second, *rest):
        out, tiles, sems = rest[-3:]
        right = jnp.concatenate([w_second[r, c] for r in range(3) for c in range(3)], axis=0)
        copies = []
        for t in range(begin, end):
            for first in range(0, PIX, 256):
                got = jnp.dot(taps_of(wide, t, first, 256), right, preferred_element_type=f32)
                rows = slice(first // S, first // S + 8)
                tiles[t - begin, rows] = (
                    fields[t, rows].astype(f32) + got.reshape(8, S, C)
                ).astype(bf16)
            copy = pltpu.make_async_copy(
                tiles.at[t - begin], out.at[t], sems.at[t - begin]
            )
            copy.start()
            copies.append(copy)
        for copy in copies:
            copy.wait()

    return body


def move(x=0, y=0, z=0):
    return 1 | (y << 1) | ((z >> 1) << 3) | (x << 5) | ((z & 1) << 7)


def parity(value):
    return bin(value).count("1") & 1


def dual(basis):
    size = len(basis)
    rows = [[(m >> k) & 1 for k in range(size)] + [int(k == i) for k in range(size)] for i, m in enumerate(basis)]
    for c in range(size):
        pivot = next(r for r in range(c, size) if rows[r][c])
        rows[c], rows[pivot] = rows[pivot], rows[c]
        for r in range(size):
            if r != c and rows[r][c]:
                rows[r] = [p ^ q for p, q in zip(rows[r], rows[c])]
    return [sum(rows[k][size + i] << k for k in range(size)) for i in range(size)]


CORE = 1
ALONG_X = [move(x=1), move(x=3)]
ALONG_Y = [move(y=1), move(y=3)]
ALONG_Z = [move(z=1), move(z=2), move(z=7)]
MOVES = ([CORE] + ALONG_X + ALONG_Y + ALONG_Z, [CORE] + ALONG_Y + ALONG_X + ALONG_Z)
DUALS = tuple(dual(m) for m in MOVES)


def place_bits(index):
    def bit(mask):
        v = index & mask
        v = v ^ (v >> 4)
        v = v ^ (v >> 2)
        return ((v ^ (v >> 1)) & 1) == 1

    half = bit(DUALS[0][0])
    bits = [half]
    for i in range(1, 5):
        bits.append(jnp.where(half, bit(DUALS[1][i]), bit(DUALS[0][i])))
    return bits


def exchange(value, ids):
    pairs = []
    for index in range(256):
        half = parity(index & DUALS[0][0])
        target = index
        for i in ids:
            target ^= MOVES[half][i]
        pairs.append((index, target))
    return lax.ppermute(value, MESH, pairs)


def pick(chunks, bits, flips):
    if not bits:
        return chunks[0]
    half = len(chunks) // 2
    low = pick(chunks[:half], bits[1:], flips[1:])
    high = pick(chunks[half:], bits[1:], flips[1:])
    return jnp.where(bits[0], low, high) if flips[0] else jnp.where(bits[0], high, low)


SUBSETS = {1: [(1,)], 2: [(1, 1), (0, 1), (1, 0)]}


def named(ids, flips):
    return tuple(i for i, f in zip(ids, flips) if f)


def scatter(value, ids, bits):
    parts = 1 << len(ids)
    rows = value.shape[0] // parts
    chunks = [value[i * rows : (i + 1) * rows] for i in range(parts)]
    mine = [bits[i] for i in ids]
    got = [
        exchange(pick(chunks, mine, flips).astype(bf16), named(ids, flips))
        for flips in SUBSETS[len(ids)]
    ]
    out = pick(chunks, mine, (0,) * len(ids))
    for part in got:
        out = out + part.astype(f32)
    return out


def spread(value, ids):
    if len(ids) == 1:
        return value + exchange(value, ids)
    a, b = ids
    both, second, first = exchange(value, ids), exchange(value, (b,)), exchange(value, (a,))
    return (value + first) + (second + both)


def gather(value, ids, bits):
    got = {(0,) * len(ids): value}
    for flips in SUBSETS[len(ids)]:
        got[flips] = exchange(value, named(ids, flips))
    mine = [bits[i] for i in ids]
    parts = [got[key] for key in sorted(got)]
    return jnp.concatenate([pick(parts, mine, key) for key in sorted(got)])


def sum_everywhere(first, second, scale, bits, pieces):
    half = bits[0]
    value = jnp.where(half, second, first) + exchange(jnp.where(half, first, second), (0,))
    value = scatter(value, (1, 2), bits)
    done = pieces(None, 0)
    value, done = lax.optimization_barrier((value, done))
    value = scatter(value, (3, 4), bits)
    done = pieces(done, 1)
    value, done = lax.optimization_barrier((value, done))
    value = spread(value, (5, 6))
    value = spread(value, (7,))
    value = (value * scale).astype(bf16)
    value = gather(value, (3, 4), bits)
    value = gather(value, (1, 2), bits).reshape(3, 3, C, C)
    other = exchange(value, (0,))
    return (
        jnp.where(half, other, value).astype(f32),
        jnp.where(half, value, other).astype(f32),
        done,
    )


def local(fields, cotangent, w_first, w_second, tile_links):
    count = lax.axis_size("space")
    own = lax.axis_index("space").astype(jnp.int32)
    bits = place_bits(lax.axis_index("dp").astype(jnp.int32) * count + own)
    own, *bits = lax.optimization_barrier((own, *bits))
    own = own.reshape(1)
    up = [(i, (i + 1) % count) for i in range(count)]
    down = [(j, i) for i, j in up]
    table, low, high, rim, x, cot, w_second = call(
        make_edges_body(count),
        [
            shape((36, 2), jnp.int32),
            shape((T, SEND, C), bf16),
            shape((T, SEND, C), bf16),
            shape((16 * RIM, C), f32),
            shape((T, S, S, C), bf16),
            shape((T, S, S, C), bf16),
            shape((3, 3, C, C), bf16),
        ],
        "shhhh",
        [
            pltpu.VMEM((16 * S, C), f32),
            pltpu.VMEM((16 * 64, C), f32),
            pltpu.VMEM((16 * S, C), f32),
            pltpu.SMEM((T, 4, 5), jnp.int32),
            pltpu.SemaphoreType.DMA((4,)),
        ],
        outs_in="svvvvvv",
    )(
        own,
        *[
            pltpu.with_memory_space_constraint(v, pltpu.HBM)
            for v in (
                tile_links,
                fields.reshape(T, S, S, C),
                cotangent.reshape(T, S, S, C),
                w_second,
            )
        ],
    )
    from_low = lax.ppermute(high, "space", up)
    from_high = lax.ppermute(low, "space", down)
    (interior,) = call(
        conv_back_body,
        [shape((T, PIX, C), f32)],
        "vv",
        [pltpu.VMEM((T, PAD, C), f32), pltpu.VMEM((T, WIDE, 3 * C), bf16)],
    )(cot, w_second)
    active, hidden_grad, wide, act_low, act_high = call(
        forward_body,
        [
            shape((T, S, S, C), bf16),
            shape((T, PIX, C), bf16),
            shape((T, WIDE, 3 * C), bf16),
            shape((T, S, C), bf16),
            shape((T, S, C), bf16),
        ],
        "svvvvvv",
        [
            pltpu.VMEM((T, PAD, C), f32),
            pltpu.VMEM((24 * S, C), f32),
            pltpu.VMEM((24 * RIM, C), f32),
            pltpu.VMEM((T, PIX, C), f32),
            pltpu.VMEM((PIX, C), f32),
            pltpu.VMEM((4 * S, C), f32),
        ],
    )(table, x, from_low, from_high, rim, interior, w_first)
    act_from_low = lax.ppermute(act_high, "space", up)
    act_from_high = lax.ppermute(act_low, "space", down)
    (grad_first,) = call(
        first_grad_body, [shape((9 * C, C), f32)], "vv", [pltpu.VMEM((C, 9 * C), f32)]
    )(hidden_grad, wide)
    grad_second, wide_active = call(
        second_grad_body,
        [shape((9 * C, C), f32), shape((T, WIDE, 3 * C), bf16)],
        "svvvv",
        [
            pltpu.VMEM((T, PAD, C), f32),
            pltpu.VMEM((24 * S, C), f32),
            pltpu.VMEM((C, 9 * C), f32),
        ],
    )(table, active, act_from_low, act_from_high, cot)

    def mixed_piece(before, n):
        args = (x, wide_active, w_second) + (() if before is None else (before,))
        (mixed,) = call(
            make_mixed_body(2 * n, 2 * n + 2),
            [shape((T, S, S, C), bf16)],
            "vvvh"[: len(args)],
            [
                pltpu.VMEM((2, S, S, C), bf16),
                pltpu.SemaphoreType.DMA((2,)),
            ],
            outs_in="h",
            aliases={} if before is None else {3: 0},
        )(*args)
        return mixed

    total = lax.axis_size("dp") * count * T * PIX
    first, second, mixed = sum_everywhere(
        grad_first, grad_second, float(total) ** -0.5, bits, mixed_piece
    )
    return (
        mixed.reshape(fields.shape),
        first,
        second,
    )


def solution(mesh):
    placed = (
        P("dp", "space", None, None, None),
        P("dp", "space", None, None, None),
        P(),
        P(),
        P("space", None, None),
    )
    return jax.shard_map(
        local,
        mesh=mesh,
        in_specs=placed,
        out_specs=(P("dp", "space", None, None, None), P(), P()),
        check_vma=False,
    )
```

```python
import jax
import jax.numpy as jnp
from jax import lax
from jax.experimental import pallas as pl
from jax.experimental.pallas import tpu as pltpu
from jax.sharding import PartitionSpec as P

f32 = jnp.float32
bf16 = jnp.bfloat16
S = 32
C = 128
T = 4
PIX = S * S
GAP = 48
LEAD = 8
PAD = (S + 2) * GAP
WIDE = (S + 2) * S
RIM = 48
SEND = S + RIM
MESH = ("dp", "space")


def vmem():
    return pl.BlockSpec(memory_space=pltpu.VMEM)


def smem():
    return pl.BlockSpec(memory_space=pltpu.SMEM)


def hbm():
    return pl.BlockSpec(memory_space=pltpu.HBM)


SPACES = {"s": smem, "v": vmem, "h": hbm}


def call(body, outs, ins, scratch=(), outs_in="", aliases={}, limit=16):
    return pl.pallas_call(
        body,
        out_shape=outs,
        in_specs=[SPACES[k]() for k in ins],
        out_specs=[SPACES[k]() for k in outs_in or "v" * len(outs)],
        scratch_shapes=list(scratch),
        input_output_aliases=aliases,
        compiler_params=pltpu.CompilerParams(vmem_limit_bytes=limit << 20),
    )


def shape(dims, dtype):
    return jax.ShapeDtypeStruct(dims, dtype)


def flip8(block):
    row = lax.broadcasted_iota(jnp.int32, (8, C), 0)
    block = pltpu.roll(block, 4, 0)
    block = jnp.where((row & 2) == 0, pltpu.roll(block, 6, 0), pltpu.roll(block, 2, 0))
    return jnp.where((row & 1) == 0, pltpu.roll(block, 7, 0), pltpu.roll(block, 1, 0))


def flip_line(line):
    parts = [line[8 * i : 8 * i + 8] for i in range(S // 8)]
    return jnp.concatenate([flip8(part) for part in reversed(parts)], axis=0)


def directed(line, flag):
    return jnp.where(jnp.full(line.shape, flag, jnp.int32) == 1, flip_line(line), line)


def link_table(own, links, table, count):
    zero = jnp.int32(0)

    def where_is(source):
        gap = (source >> 2) - own + 1
        gap = jnp.where(gap < 0, gap + count, gap)
        return jnp.where(gap >= count, gap - count, gap), source & 3

    sides = []
    facing = {(way, slot): zero for way in (0, 2) for slot in range(T)}
    for n in range(4 * T):
        rel, slot = where_is(links[n // 4, n % 4, 0])
        edge = links[n // 4, n % 4, 1]
        sides.append((rel, slot, edge))
        for way in (0, 2):
            for s in range(T):
                facing[way, s] += jnp.where((rel == way) & (slot == s), edge, zero)
    for n, (rel, slot, edge) in enumerate(sides):
        line = jnp.where(rel == 1, slot * 4 + edge, jnp.where(rel == 0, 16 + slot, 20 + slot))
        table[n, 0] = line
        table[n, 1] = links[n // 4, n % 4, 2]
    for n in range(4 * T):
        rel, slot = where_is(links[n // 4, n % 4, 3])
        at = links[n // 4, n % 4, 4]
        low, high = zero, zero
        for s in range(T):
            low += jnp.where(slot == s, facing[0, s], zero)
            high += jnp.where(slot == s, facing[2, s], zero)
        face = jnp.where(rel == 0, low, high)
        start = jnp.where(face == 1, 1, jnp.where(face == 2, 3, 0))
        near = slot * 4 + jnp.where(at < 2, 0, 2)
        line = jnp.where(rel == 1, near, jnp.where(rel == 0, 16 + slot, 20 + slot))
        far_end = jnp.where(at == start, 0, 1)
        near_end = jnp.where((at == 1) | (at == 2), 1, 0)
        table[16 + n, 0] = line
        table[16 + n, 1] = jnp.where(rel == 1, near_end, far_end)
    faces = []
    for t in range(T):
        low, high = zero, zero
        for k in range(4):
            rel = sides[t * 4 + k][0]
            low += jnp.where(rel == 0, k, 0)
            high += jnp.where(rel == 2, k, 0)
        table[32 + t, 0] = low
        table[32 + t, 1] = high
        faces.append((low, high))
    return faces


def make_edges_body(count):
    def body(
        own, tile_links, fields_far, cot_far, w_second_far,
        table, low, high, rim, fields, cot, w_second,
        lines, wide, slab, links, sems,
    ):
        copies = [
            pltpu.make_async_copy(source, target, sems.at[n])
            for n, (source, target) in enumerate(
                (
                    (tile_links, links),
                    (cot_far, cot),
                    (w_second_far, w_second),
                    (fields_far, fields),
                )
            )
        ]
        for copy in copies:
            copy.start()
        wide[...] = jnp.zeros(wide.shape, f32)
        copies[0].wait()
        faces = link_table(own[0], links, table, count)

        def put_lines(source, t, store):
            store(0, source[t, 0].astype(f32))
            store(2, source[t, S - 1].astype(f32))
            for edge, first, at in ((3, 0, 0), (1, 16, 15)):
                slab[...] = source[t, :, first : first + 16, :].astype(f32).reshape(16 * S, C)
                store(edge, slab[pl.ds(at, S, stride=16), :])

        copies[1].wait()
        for t in range(T):

            def store(k, line, t=t):
                wide[(k * T + t) * 64 + 16 : (k * T + t) * 64 + 16 + S, :] = line

            put_lines(cot, t, store)
        taps = {
            0: [(0, c) for c in range(3)],
            1: [(r, 2) for r in range(3)],
            2: [(2, c) for c in range(3)],
            3: [(r, 0) for r in range(3)],
        }
        copies[2].wait()
        for k in range(4):
            left = []
            for t in range(T):
                base = (k * T + t) * 64
                left.append(
                    jnp.concatenate(
                        [wide[base + 9 - c : base + 9 - c + RIM, :].astype(bf16) for c in range(3)],
                        axis=1,
                    )
                )
            left = jnp.concatenate(left, axis=0)
            right = jnp.concatenate([w_second[r, c] for r, c in taps[k]], axis=1)
            out = lax.dot_general(
                left, right, (((1,), (1,)), ((), ())), preferred_element_type=f32
            )
            for t in range(T):
                rim[(t * 4 + k) * RIM : (t * 4 + k + 1) * RIM, :] = out[t * RIM : (t + 1) * RIM]
        copies[3].wait()
        for t in range(T):

            def store(k, line, t=t):
                lines[(t * 4 + k) * S : (t * 4 + k + 1) * S, :] = line

            put_lines(fields, t, store)
        for t in range(T):
            for out_ref, face in zip((low, high), faces[t]):
                n = t * 4 + face
                at = pl.multiple_of(n * S, S)
                out_ref[t, 0:S, :] = lines[pl.ds(at, S), :].astype(bf16)
                at = pl.multiple_of(n * RIM, 16)
                out_ref[t, S:SEND, :] = rim[pl.ds(at, RIM), :].astype(bf16)

    return body


def widen(padded, t, wide):
    for p in range(S + 2):
        for c in range(3):
            at = p * GAP + LEAD - 1 + c
            wide[t, p * S : (p + 1) * S, c * C : (c + 1) * C] = padded[t, at : at + S, :].astype(bf16)


def taps_of(wide, t, first, rows):
    return jnp.concatenate(
        [wide[t, r * S + first : r * S + first + rows, :] for r in range(3)], axis=1
    )


def pair_taps(wide, t, first, pairs):
    parts = []
    for r in range(4):
        parts.append(
            jnp.concatenate(
                [wide[t, (2 * p + r) * S : (2 * p + r + 1) * S, :] for p in range(first, first + pairs)],
                axis=0,
            )
        )
    return jnp.concatenate(parts, axis=1)


def pair_kernel(tap):
    zero = jnp.zeros((C, C), bf16)
    rows = []
    for r in range(4):
        for c in range(3):
            even = tap(r, c) if r < 3 else zero
            odd = tap(r - 1, c) if r > 0 else zero
            rows.append(jnp.concatenate([even, odd], axis=1))
    return jnp.concatenate(rows, axis=0)


def pair_conv(wide, t, first, pairs, right):
    got = jnp.dot(pair_taps(wide, t, first, pairs), right, preferred_element_type=f32)
    for p in range(pairs):
        for odd in range(2):
            yield 2 * (first + p) + odd, got[p * S : (p + 1) * S, odd * C : (odd + 1) * C]


def put_interior(source, padded, t):
    for r in range(S):
        at = (1 + r) * GAP + LEAD
        padded[t, at : at + S, :] = source[t, r].astype(f32)


def conv_back_body(cot, w_second, out, padded, wide, right):
    right[...] = pair_kernel(lambda r, c: w_second[2 - r, 2 - c].T)
    zero = jnp.zeros((GAP, C), f32)
    for t in range(T):
        padded[t, 0:GAP, :] = zero
        padded[t, PAD - GAP : PAD, :] = zero
        for r in range(S):
            at = (1 + r) * GAP
            padded[t, at : at + 8, :] = zero[:8]
            padded[t, at + LEAD + S : at + GAP, :] = zero[:8]
        put_interior(cot, padded, t)
        widen(padded, t, wide)
        for first in range(0, S // 2, 8):
            for row, value in pair_conv(wide, t, first, 8, right[...]):
                out[t, row * S : (row + 1) * S, :] = value


def collect_lines(padded, lines, low, high):
    for t in range(T):
        base = GAP + LEAD
        spots = {
            0: padded[t, base : base + S, :],
            1: padded[t, pl.ds(base + S - 1, S, stride=GAP), :],
            2: padded[t, base + (S - 1) * GAP : base + (S - 1) * GAP + S, :],
            3: padded[t, pl.ds(base, S, stride=GAP), :],
        }
        for k in range(4):
            lines[(t * 4 + k) * S : (t * 4 + k + 1) * S, :] = spots[k]
        for first, received in ((16, low), (20, high)):
            lines[(first + t) * S : (first + t + 1) * S, :] = received[t, 0:S, :].astype(f32)


def put_rims(table, lines, padded):
    for t in range(T):
        for k in range(4):
            n = t * 4 + k
            at = pl.multiple_of(table[n, 0] * S, S)
            line = directed(lines[pl.ds(at, S), :], table[n, 1])
            if k == 0:
                padded[t, LEAD : LEAD + S, :] = line
            elif k == 2:
                at = (S + 1) * GAP + LEAD
                padded[t, at : at + S, :] = line
            elif k == 1:
                padded[t, pl.ds(GAP + LEAD + S, S, stride=GAP), :] = line
            else:
                padded[t, pl.ds(GAP + LEAD - 1, S, stride=GAP), :] = line
        for k, spot in enumerate(
            (
                LEAD - 1,
                LEAD + S,
                (S + 1) * GAP + LEAD + S,
                (S + 1) * GAP + LEAD - 1,
            )
        ):
            n = 16 + t * 4 + k
            at = table[n, 0] * S + table[n, 1] * (S - 1)
            padded[t, spot : spot + 1, :] = lines[pl.ds(at, 1), :]


def forward_body(
    table, fields, low, high, rim, interior, w_first,
    active, hidden_grad, wide, send_low, send_high,
    padded, lines, rims, grads, rounded, edges, right,
):
    for t in range(T):
        put_interior(fields, padded, t)
    collect_lines(padded, lines, low, high)
    put_rims(table, lines, padded)
    rims[0 : 16 * RIM, :] = rim[...]
    for t in range(T):
        rims[(16 + t) * RIM : (17 + t) * RIM, :] = low[t, S:SEND, :].astype(f32)
        rims[(20 + t) * RIM : (21 + t) * RIM, :] = high[t, S:SEND, :].astype(f32)
    for t in range(T):
        grads[t] = interior[t]
        for k in range(4):
            n = t * 4 + k
            at = pl.multiple_of(table[n, 0] * RIM, 16)
            line = directed(rims[pl.ds(at + 8, S), :], table[n, 1])
            if k == 0:
                grads[t, 0:S, :] += line
            elif k == 2:
                grads[t, PIX - S : PIX, :] += line
            else:
                spot = pl.ds(S - 1 if k == 1 else 0, S, stride=S)
                grads[t, spot, :] = grads[t, spot, :] + line
        for k, spot in enumerate((0, S - 1, PIX - 1, PIX - S)):
            n = 16 + t * 4 + k
            at = table[n, 0] * RIM + 7 + table[n, 1] * (S + 1)
            grads[t, spot : spot + 1, :] += rims[pl.ds(at, 1), :]
    right[...] = pair_kernel(lambda r, c: w_first[r, c])

    for t in range(T):
        widen(padded, t, wide)
        for first in range(0, S // 2, 8):
            for row, hidden in pair_conv(wide, t, first, 8, right[...]):
                gate = 1.0 / (1.0 + jnp.exp(-hidden))
                act = (hidden * gate).astype(bf16)
                active[t, row] = act
                span = slice(row * S, (row + 1) * S)
                rounded[t, span, :] = act.astype(f32)
                hidden_grad[t, span, :] = (
                    grads[t, span, :] * gate * (1.0 + hidden * (1.0 - gate))
                ).astype(bf16)
    for t in range(T):
        edges[t, 0:S, :] = rounded[t, 0:S, :]
        edges[t, S : 2 * S, :] = rounded[t, pl.ds(S - 1, S, stride=S), :]
        edges[t, 2 * S : 3 * S, :] = rounded[t, PIX - S : PIX, :]
        edges[t, 3 * S : 4 * S, :] = rounded[t, pl.ds(0, S, stride=S), :]
        for out_ref, which in ((send_low, 0), (send_high, 1)):
            at = pl.multiple_of(table[32 + t, which] * S, S)
            out_ref[t] = edges[t, pl.ds(at, S), :].astype(bf16)


def weight_grad(cot_of, wide, acc, out):
    for t in range(T):
        got = jnp.dot(
            cot_of(t).T,
            jnp.concatenate([wide[t, r * S : r * S + PIX, :] for r in range(3)], axis=1),
            preferred_element_type=f32,
        )
        acc[...] = got if t == 0 else acc[...] + got
    for n in range(9):
        out[n * C : (n + 1) * C, :] = acc[:, n * C : (n + 1) * C].T


def first_grad_body(hidden_grad, wide, out, acc):
    weight_grad(lambda t: hidden_grad[t], wide, acc, out)


def second_grad_body(table, active, low, high, cot, out, wide, padded, lines, acc):
    for t in range(T):
        put_interior(active, padded, t)
    collect_lines(padded, lines, low, high)
    put_rims(table, lines, padded)
    for t in range(T):
        widen(padded, t, wide)
    weight_grad(lambda t: cot[t].reshape(PIX, C), wide, acc, out)


def make_mixed_body(begin, end):
    def body(fields, wide, w_second, *rest):
        out, tiles, sems, right = rest[-4:]
        right[...] = pair_kernel(lambda r, c: w_second[r, c])
        copies = []
        for t in range(begin, end):
            for first in range(0, S // 2, 8):
                for row, value in pair_conv(wide, t, first, 8, right[...]):
                    tiles[t - begin, row] = (fields[t, row].astype(f32) + value).astype(bf16)
            copy = pltpu.make_async_copy(
                tiles.at[t - begin], out.at[t], sems.at[t - begin]
            )
            copy.start()
            copies.append(copy)
        for copy in copies:
            copy.wait()

    return body


def move(x=0, y=0, z=0):
    return 1 | (y << 1) | ((z >> 1) << 3) | (x << 5) | ((z & 1) << 7)


def parity(value):
    return bin(value).count("1") & 1


def dual(basis):
    size = len(basis)
    rows = [[(m >> k) & 1 for k in range(size)] + [int(k == i) for k in range(size)] for i, m in enumerate(basis)]
    for c in range(size):
        pivot = next(r for r in range(c, size) if rows[r][c])
        rows[c], rows[pivot] = rows[pivot], rows[c]
        for r in range(size):
            if r != c and rows[r][c]:
                rows[r] = [p ^ q for p, q in zip(rows[r], rows[c])]
    return [sum(rows[k][size + i] << k for k in range(size)) for i in range(size)]


CORE = 1
ALONG_X = [move(x=1), move(x=3)]
ALONG_Y = [move(y=1), move(y=3)]
ALONG_Z = [move(z=1), move(z=2), move(z=7)]
MOVES = ([CORE] + ALONG_X + ALONG_Y + ALONG_Z, [CORE] + ALONG_Y + ALONG_X + ALONG_Z)
DUALS = tuple(dual(m) for m in MOVES)


def place_bits(index):
    def bit(mask):
        v = index & mask
        v = v ^ (v >> 4)
        v = v ^ (v >> 2)
        return ((v ^ (v >> 1)) & 1) == 1

    half = bit(DUALS[0][0])
    bits = [half]
    for i in range(1, 5):
        bits.append(jnp.where(half, bit(DUALS[1][i]), bit(DUALS[0][i])))
    return bits


def exchange(value, ids):
    pairs = []
    for index in range(256):
        half = parity(index & DUALS[0][0])
        target = index
        for i in ids:
            target ^= MOVES[half][i]
        pairs.append((index, target))
    return lax.ppermute(value, MESH, pairs)


def pick(chunks, bits, flips):
    if not bits:
        return chunks[0]
    half = len(chunks) // 2
    low = pick(chunks[:half], bits[1:], flips[1:])
    high = pick(chunks[half:], bits[1:], flips[1:])
    return jnp.where(bits[0], low, high) if flips[0] else jnp.where(bits[0], high, low)


SUBSETS = {1: [(1,)], 2: [(1, 1), (0, 1), (1, 0)]}


def named(ids, flips):
    return tuple(i for i, f in zip(ids, flips) if f)


def scatter(value, ids, bits):
    parts = 1 << len(ids)
    rows = value.shape[0] // parts
    chunks = [value[i * rows : (i + 1) * rows] for i in range(parts)]
    mine = [bits[i] for i in ids]
    got = [
        exchange(pick(chunks, mine, flips).astype(bf16), named(ids, flips))
        for flips in SUBSETS[len(ids)]
    ]
    out = pick(chunks, mine, (0,) * len(ids))
    for part in got:
        out = out + part.astype(f32)
    return out


def spread(value, ids):
    if len(ids) == 1:
        return value + exchange(value, ids)
    a, b = ids
    both, second, first = exchange(value, ids), exchange(value, (b,)), exchange(value, (a,))
    return (value + first) + (second + both)


def gather(value, ids, bits):
    got = {(0,) * len(ids): value}
    for flips in SUBSETS[len(ids)]:
        got[flips] = exchange(value, named(ids, flips))
    mine = [bits[i] for i in ids]
    parts = [got[key] for key in sorted(got)]
    return jnp.concatenate([pick(parts, mine, key) for key in sorted(got)])


def sum_everywhere(first, second, scale, bits, pieces):
    half = bits[0]
    value = jnp.where(half, second, first) + exchange(jnp.where(half, first, second), (0,))
    value = scatter(value, (1, 2), bits)
    done = pieces(None, 0)
    value, done = lax.optimization_barrier((value, done))
    value = scatter(value, (3, 4), bits)
    done = pieces(done, 1)
    value, done = lax.optimization_barrier((value, done))
    value = spread(value, (5, 6))
    value = spread(value, (7,))
    value = (value * scale).astype(bf16)
    value = gather(value, (3, 4), bits)
    value = gather(value, (1, 2), bits).reshape(3, 3, C, C)
    other = exchange(value, (0,))
    return (
        jnp.where(half, other, value).astype(f32),
        jnp.where(half, value, other).astype(f32),
        done,
    )


def local(fields, cotangent, w_first, w_second, tile_links):
    count = lax.axis_size("space")
    own = lax.axis_index("space").astype(jnp.int32)
    bits = place_bits(lax.axis_index("dp").astype(jnp.int32) * count + own)
    own, *bits = lax.optimization_barrier((own, *bits))
    own = own.reshape(1)
    up = [(i, (i + 1) % count) for i in range(count)]
    down = [(j, i) for i, j in up]
    table, low, high, rim, x, cot, w_second = call(
        make_edges_body(count),
        [
            shape((36, 2), jnp.int32),
            shape((T, SEND, C), bf16),
            shape((T, SEND, C), bf16),
            shape((16 * RIM, C), f32),
            shape((T, S, S, C), bf16),
            shape((T, S, S, C), bf16),
            shape((3, 3, C, C), bf16),
        ],
        "shhhh",
        [
            pltpu.VMEM((16 * S, C), f32),
            pltpu.VMEM((16 * 64, C), f32),
            pltpu.VMEM((16 * S, C), f32),
            pltpu.SMEM((T, 4, 5), jnp.int32),
            pltpu.SemaphoreType.DMA((4,)),
        ],
        outs_in="svvvvvv",
    )(
        own,
        *[
            pltpu.with_memory_space_constraint(v, pltpu.HBM)
            for v in (
                tile_links,
                fields.reshape(T, S, S, C),
                cotangent.reshape(T, S, S, C),
                w_second,
            )
        ],
    )
    from_low = lax.ppermute(high, "space", up)
    from_high = lax.ppermute(low, "space", down)
    (interior,) = call(
        conv_back_body,
        [shape((T, PIX, C), f32)],
        "vv",
        [
            pltpu.VMEM((T, PAD, C), f32),
            pltpu.VMEM((T, WIDE, 3 * C), bf16),
            pltpu.VMEM((12 * C, 2 * C), bf16),
        ],
    )(cot, w_second)
    active, hidden_grad, wide, act_low, act_high = call(
        forward_body,
        [
            shape((T, S, S, C), bf16),
            shape((T, PIX, C), bf16),
            shape((T, WIDE, 3 * C), bf16),
            shape((T, S, C), bf16),
            shape((T, S, C), bf16),
        ],
        "svvvvvv",
        [
            pltpu.VMEM((T, PAD, C), f32),
            pltpu.VMEM((24 * S, C), f32),
            pltpu.VMEM((24 * RIM, C), f32),
            pltpu.VMEM((T, PIX, C), f32),
            pltpu.VMEM((T, PIX, C), f32),
            pltpu.VMEM((T, 4 * S, C), f32),
            pltpu.VMEM((12 * C, 2 * C), bf16),
        ],
    )(table, x, from_low, from_high, rim, interior, w_first)
    act_from_low = lax.ppermute(act_high, "space", up)
    act_from_high = lax.ppermute(act_low, "space", down)
    (grad_first,) = call(
        first_grad_body, [shape((9 * C, C), f32)], "vv", [pltpu.VMEM((C, 9 * C), f32)]
    )(hidden_grad, wide)
    grad_second, wide_active = call(
        second_grad_body,
        [shape((9 * C, C), f32), shape((T, WIDE, 3 * C), bf16)],
        "svvvv",
        [
            pltpu.VMEM((T, PAD, C), f32),
            pltpu.VMEM((24 * S, C), f32),
            pltpu.VMEM((C, 9 * C), f32),
        ],
    )(table, active, act_from_low, act_from_high, cot)

    def mixed_piece(before, n):
        args = (x, wide_active, w_second) + (() if before is None else (before,))
        (mixed,) = call(
            make_mixed_body(2 * n, 2 * n + 2),
            [shape((T, S, S, C), bf16)],
            "vvvh"[: len(args)],
            [
                pltpu.VMEM((2, S, S, C), bf16),
                pltpu.SemaphoreType.DMA((2,)),
                pltpu.VMEM((12 * C, 2 * C), bf16),
            ],
            outs_in="h",
            aliases={} if before is None else {3: 0},
        )(*args)
        return mixed

    total = lax.axis_size("dp") * count * T * PIX
    first, second, mixed = sum_everywhere(
        grad_first, grad_second, float(total) ** -0.5, bits, mixed_piece
    )
    return (
        mixed.reshape(fields.shape),
        first,
        second,
    )


def solution(mesh):
    placed = (
        P("dp", "space", None, None, None),
        P("dp", "space", None, None, None),
        P(),
        P(),
        P("space", None, None),
    )
    return jax.shard_map(
        local,
        mesh=mesh,
        in_specs=placed,
        out_specs=(P("dp", "space", None, None, None), P(), P()),
        check_vma=False,
    )
```

```python
import jax
import jax.numpy as jnp
from jax import lax
from jax.experimental import pallas as pl
from jax.experimental.pallas import tpu as pltpu
from jax.sharding import PartitionSpec as P

f32 = jnp.float32
bf16 = jnp.bfloat16
S = 32
C = 128
T = 4
PIX = S * S
GAP = 48
LEAD = 8
PAD = (S + 2) * GAP
WIDE = (S + 2) * S
RIM = 48
SEND = S + RIM
MESH = ("dp", "space")


def vmem():
    return pl.BlockSpec(memory_space=pltpu.VMEM)


def smem():
    return pl.BlockSpec(memory_space=pltpu.SMEM)


def hbm():
    return pl.BlockSpec(memory_space=pltpu.HBM)


SPACES = {"s": smem, "v": vmem, "h": hbm}


def call(body, outs, ins, scratch=(), outs_in="", aliases={}, limit=16):
    return pl.pallas_call(
        body,
        out_shape=outs,
        in_specs=[SPACES[k]() for k in ins],
        out_specs=[SPACES[k]() for k in outs_in or "v" * len(outs)],
        scratch_shapes=list(scratch),
        input_output_aliases=aliases,
        compiler_params=pltpu.CompilerParams(vmem_limit_bytes=limit << 20),
    )


def shape(dims, dtype):
    return jax.ShapeDtypeStruct(dims, dtype)


def flip8(block):
    row = lax.broadcasted_iota(jnp.int32, (8, C), 0)
    block = pltpu.roll(block, 4, 0)
    block = jnp.where((row & 2) == 0, pltpu.roll(block, 6, 0), pltpu.roll(block, 2, 0))
    return jnp.where((row & 1) == 0, pltpu.roll(block, 7, 0), pltpu.roll(block, 1, 0))


def flip_line(line):
    parts = [line[8 * i : 8 * i + 8] for i in range(S // 8)]
    return jnp.concatenate([flip8(part) for part in reversed(parts)], axis=0)


def directed(line, flag):
    return jnp.where(jnp.full(line.shape, flag, jnp.int32) == 1, flip_line(line), line)


def link_table(own, links, table, count):
    zero = jnp.int32(0)

    def where_is(source):
        gap = (source >> 2) - own + 1
        gap = jnp.where(gap < 0, gap + count, gap)
        return jnp.where(gap >= count, gap - count, gap), source & 3

    sides = []
    facing = {(way, slot): zero for way in (0, 2) for slot in range(T)}
    for n in range(4 * T):
        rel, slot = where_is(links[n // 4, n % 4, 0])
        edge = links[n // 4, n % 4, 1]
        sides.append((rel, slot, edge))
        for way in (0, 2):
            for s in range(T):
                facing[way, s] += jnp.where((rel == way) & (slot == s), edge, zero)
    odd = (own & 1) == 1
    below = jnp.where(odd, 16, 20)
    above = jnp.where(odd, 20, 16)
    for n, (rel, slot, edge) in enumerate(sides):
        line = jnp.where(rel == 1, slot * 4 + edge, jnp.where(rel == 0, below, above) + slot)
        table[n, 0] = line
        table[n, 1] = links[n // 4, n % 4, 2]
    for n in range(4 * T):
        rel, slot = where_is(links[n // 4, n % 4, 3])
        at = links[n // 4, n % 4, 4]
        low, high = zero, zero
        for s in range(T):
            low += jnp.where(slot == s, facing[0, s], zero)
            high += jnp.where(slot == s, facing[2, s], zero)
        face = jnp.where(rel == 0, low, high)
        start = jnp.where(face == 1, 1, jnp.where(face == 2, 3, 0))
        near = slot * 4 + jnp.where(at < 2, 0, 2)
        line = jnp.where(rel == 1, near, jnp.where(rel == 0, below, above) + slot)
        far_end = jnp.where(at == start, 0, 1)
        near_end = jnp.where((at == 1) | (at == 2), 1, 0)
        table[16 + n, 0] = line
        table[16 + n, 1] = jnp.where(rel == 1, near_end, far_end)
    faces = []
    for t in range(T):
        low, high = zero, zero
        for k in range(4):
            rel = sides[t * 4 + k][0]
            low += jnp.where(rel == 0, k, 0)
            high += jnp.where(rel == 2, k, 0)
        low, high = jnp.where(odd, low, high), jnp.where(odd, high, low)
        table[32 + t, 0] = low
        table[32 + t, 1] = high
        faces.append((low, high))
    return faces


def make_edges_body(count):
    def body(
        own, tile_links, fields_far, cot_far, w_second_far,
        table, near, far, rim, fields, cot, w_second,
        lines, wide, slab, links, sems,
    ):
        copies = [
            pltpu.make_async_copy(source, target, sems.at[n])
            for n, (source, target) in enumerate(
                (
                    (tile_links, links),
                    (cot_far, cot),
                    (w_second_far, w_second),
                    (fields_far, fields),
                )
            )
        ]
        for copy in copies:
            copy.start()
        wide[...] = jnp.zeros(wide.shape, f32)
        copies[0].wait()
        faces = link_table(own[0], links, table, count)

        def put_lines(source, t, store):
            store(0, source[t, 0].astype(f32))
            store(2, source[t, S - 1].astype(f32))
            for edge, first, at in ((3, 0, 0), (1, 16, 15)):
                slab[...] = source[t, :, first : first + 16, :].astype(f32).reshape(16 * S, C)
                store(edge, slab[pl.ds(at, S, stride=16), :])

        copies[1].wait()
        for t in range(T):

            def store(k, line, t=t):
                wide[(k * T + t) * 64 + 16 : (k * T + t) * 64 + 16 + S, :] = line

            put_lines(cot, t, store)
        taps = {
            0: [(0, c) for c in range(3)],
            1: [(r, 2) for r in range(3)],
            2: [(2, c) for c in range(3)],
            3: [(r, 0) for r in range(3)],
        }
        copies[2].wait()
        for k in range(4):
            left = []
            for t in range(T):
                base = (k * T + t) * 64
                left.append(
                    jnp.concatenate(
                        [wide[base + 9 - c : base + 9 - c + RIM, :].astype(bf16) for c in range(3)],
                        axis=1,
                    )
                )
            left = jnp.concatenate(left, axis=0)
            right = jnp.concatenate([w_second[r, c] for r, c in taps[k]], axis=1)
            out = lax.dot_general(
                left, right, (((1,), (1,)), ((), ())), preferred_element_type=f32
            )
            for t in range(T):
                rim[(t * 4 + k) * RIM : (t * 4 + k + 1) * RIM, :] = out[t * RIM : (t + 1) * RIM]
        copies[3].wait()
        for t in range(T):

            def store(k, line, t=t):
                lines[(t * 4 + k) * S : (t * 4 + k + 1) * S, :] = line

            put_lines(fields, t, store)
        for t in range(T):
            for out_ref, face in zip((near, far), faces[t]):
                n = t * 4 + face
                at = pl.multiple_of(n * S, S)
                out_ref[t, 0:S, :] = lines[pl.ds(at, S), :].astype(bf16)
                at = pl.multiple_of(n * RIM, 16)
                out_ref[t, S:SEND, :] = rim[pl.ds(at, RIM), :].astype(bf16)

    return body


def widen(padded, t, wide):
    for p in range(S + 2):
        for c in range(3):
            at = p * GAP + LEAD - 1 + c
            wide[t, p * S : (p + 1) * S, c * C : (c + 1) * C] = padded[t, at : at + S, :].astype(bf16)


def taps_of(wide, t, first, rows):
    return jnp.concatenate(
        [wide[t, r * S + first : r * S + first + rows, :] for r in range(3)], axis=1
    )


def pair_taps(wide, t, first, pairs):
    parts = []
    for r in range(4):
        parts.append(
            jnp.concatenate(
                [wide[t, (2 * p + r) * S : (2 * p + r + 1) * S, :] for p in range(first, first + pairs)],
                axis=0,
            )
        )
    return jnp.concatenate(parts, axis=1)


def pair_kernel(tap):
    zero = jnp.zeros((C, C), bf16)
    rows = []
    for r in range(4):
        for c in range(3):
            even = tap(r, c) if r < 3 else zero
            odd = tap(r - 1, c) if r > 0 else zero
            rows.append(jnp.concatenate([even, odd], axis=1))
    return jnp.concatenate(rows, axis=0)


def pair_conv(wide, t, first, pairs, right):
    got = jnp.dot(pair_taps(wide, t, first, pairs), right, preferred_element_type=f32)
    for p in range(pairs):
        for odd in range(2):
            yield 2 * (first + p) + odd, got[p * S : (p + 1) * S, odd * C : (odd + 1) * C]


def put_interior(source, padded, t):
    for r in range(S):
        at = (1 + r) * GAP + LEAD
        padded[t, at : at + S, :] = source[t, r].astype(f32)


def conv_back_body(cot, w_second, fields, out, padded_fields, padded, wide, right):
    for t in range(T):
        put_interior(fields, padded_fields, t)
    right[...] = pair_kernel(lambda r, c: w_second[2 - r, 2 - c].T)
    zero = jnp.zeros((GAP, C), f32)
    for t in range(T):
        padded[t, 0:GAP, :] = zero
        padded[t, PAD - GAP : PAD, :] = zero
        for r in range(S):
            at = (1 + r) * GAP
            padded[t, at : at + 8, :] = zero[:8]
            padded[t, at + LEAD + S : at + GAP, :] = zero[:8]
        put_interior(cot, padded, t)
        widen(padded, t, wide)
        for first in range(0, S // 2, 8):
            for row, value in pair_conv(wide, t, first, 8, right[...]):
                out[t, row * S : (row + 1) * S, :] = value


def collect_lines(padded, lines, near, far):
    for t in range(T):
        base = GAP + LEAD
        spots = {
            0: padded[t, base : base + S, :],
            1: padded[t, pl.ds(base + S - 1, S, stride=GAP), :],
            2: padded[t, base + (S - 1) * GAP : base + (S - 1) * GAP + S, :],
            3: padded[t, pl.ds(base, S, stride=GAP), :],
        }
        for k in range(4):
            lines[(t * 4 + k) * S : (t * 4 + k + 1) * S, :] = spots[k]
        for first, received in ((16, near), (20, far)):
            lines[(first + t) * S : (first + t + 1) * S, :] = received[t, 0:S, :].astype(f32)


def put_rims(table, lines, padded):
    for t in range(T):
        for k in range(4):
            n = t * 4 + k
            at = pl.multiple_of(table[n, 0] * S, S)
            line = directed(lines[pl.ds(at, S), :], table[n, 1])
            if k == 0:
                padded[t, LEAD : LEAD + S, :] = line
            elif k == 2:
                at = (S + 1) * GAP + LEAD
                padded[t, at : at + S, :] = line
            elif k == 1:
                padded[t, pl.ds(GAP + LEAD + S, S, stride=GAP), :] = line
            else:
                padded[t, pl.ds(GAP + LEAD - 1, S, stride=GAP), :] = line
        for k, spot in enumerate(
            (
                LEAD - 1,
                LEAD + S,
                (S + 1) * GAP + LEAD + S,
                (S + 1) * GAP + LEAD - 1,
            )
        ):
            n = 16 + t * 4 + k
            at = table[n, 0] * S + table[n, 1] * (S - 1)
            padded[t, spot : spot + 1, :] = lines[pl.ds(at, 1), :]


def forward_body(
    table, padded_in, near, far, rim, interior, w_first,
    active, hidden_grad, wide, send_near, send_far, padded, grads,
    lines, rims, rounded, edges, right,
):
    collect_lines(padded, lines, near, far)
    put_rims(table, lines, padded)
    rims[0 : 16 * RIM, :] = rim[...]
    for t in range(T):
        rims[(16 + t) * RIM : (17 + t) * RIM, :] = near[t, S:SEND, :].astype(f32)
        rims[(20 + t) * RIM : (21 + t) * RIM, :] = far[t, S:SEND, :].astype(f32)
    for t in range(T):
        for k in range(4):
            n = t * 4 + k
            at = pl.multiple_of(table[n, 0] * RIM, 16)
            line = directed(rims[pl.ds(at + 8, S), :], table[n, 1])
            if k == 0:
                grads[t, 0:S, :] += line
            elif k == 2:
                grads[t, PIX - S : PIX, :] += line
            else:
                spot = pl.ds(S - 1 if k == 1 else 0, S, stride=S)
                grads[t, spot, :] = grads[t, spot, :] + line
        for k, spot in enumerate((0, S - 1, PIX - 1, PIX - S)):
            n = 16 + t * 4 + k
            at = table[n, 0] * RIM + 7 + table[n, 1] * (S + 1)
            grads[t, spot : spot + 1, :] += rims[pl.ds(at, 1), :]
    right[...] = pair_kernel(lambda r, c: w_first[r, c])

    for t in range(T):
        widen(padded, t, wide)
        for first in range(0, S // 2, 8):
            for row, hidden in pair_conv(wide, t, first, 8, right[...]):
                gate = 1.0 / (1.0 + jnp.exp(-hidden))
                act = (hidden * gate).astype(bf16)
                active[t, row] = act
                span = slice(row * S, (row + 1) * S)
                rounded[t, span, :] = act.astype(f32)
                hidden_grad[t, span, :] = (
                    grads[t, span, :] * gate * (1.0 + hidden * (1.0 - gate))
                ).astype(bf16)
    for t in range(T):
        edges[t, 0:S, :] = rounded[t, 0:S, :]
        edges[t, S : 2 * S, :] = rounded[t, pl.ds(S - 1, S, stride=S), :]
        edges[t, 2 * S : 3 * S, :] = rounded[t, PIX - S : PIX, :]
        edges[t, 3 * S : 4 * S, :] = rounded[t, pl.ds(0, S, stride=S), :]
        for out_ref, which in ((send_near, 0), (send_far, 1)):
            at = pl.multiple_of(table[32 + t, which] * S, S)
            out_ref[t] = edges[t, pl.ds(at, S), :].astype(bf16)


def weight_grad(cot_of, wide, acc, out):
    for t in range(T):
        got = jnp.dot(
            cot_of(t),
            jnp.concatenate([wide[t, r * S : r * S + PIX, :] for r in range(3)], axis=1),
            preferred_element_type=f32,
        )
        acc[...] = got if t == 0 else acc[...] + got
    for n in range(9):
        out[n * C : (n + 1) * C, :] = acc[:, n * C : (n + 1) * C].T


def first_grad_body(hidden_grad, wide, active, cot, out, padded, turned, acc):
    weight_grad(lambda t: hidden_grad[t].T, wide, acc, out)
    for t in range(T):
        put_interior(active, padded, t)
        turned[t] = cot[t].reshape(PIX, C).T


def second_grad_body(table, padded_in, near, far, turned, out, wide, padded, lines, acc):
    collect_lines(padded, lines, near, far)
    put_rims(table, lines, padded)
    for t in range(T):
        widen(padded, t, wide)
    weight_grad(lambda t: turned[t], wide, acc, out)


def make_mixed_body(begin, end):
    def body(fields, wide, w_second, *rest):
        out, tiles, sems, right = rest[-4:]
        right[...] = pair_kernel(lambda r, c: w_second[r, c])
        copies = []
        for t in range(begin, end):
            for first in range(0, S // 2, 8):
                for row, value in pair_conv(wide, t, first, 8, right[...]):
                    tiles[t - begin, row] = (fields[t, row].astype(f32) + value).astype(bf16)
            copy = pltpu.make_async_copy(
                tiles.at[t - begin], out.at[t], sems.at[t - begin]
            )
            copy.start()
            copies.append(copy)
        for copy in copies:
            copy.wait()

    return body


def move(x=0, y=0, z=0):
    return 1 | (y << 1) | ((z >> 1) << 3) | (x << 5) | ((z & 1) << 7)


def parity(value):
    return bin(value).count("1") & 1


def dual(basis):
    size = len(basis)
    rows = [[(m >> k) & 1 for k in range(size)] + [int(k == i) for k in range(size)] for i, m in enumerate(basis)]
    for c in range(size):
        pivot = next(r for r in range(c, size) if rows[r][c])
        rows[c], rows[pivot] = rows[pivot], rows[c]
        for r in range(size):
            if r != c and rows[r][c]:
                rows[r] = [p ^ q for p, q in zip(rows[r], rows[c])]
    return [sum(rows[k][size + i] << k for k in range(size)) for i in range(size)]


CORE = 1
ALONG_X = [move(x=1), move(x=3)]
ALONG_Y = [move(y=1), move(y=3)]
ALONG_Z = [move(z=1), move(z=2), move(z=7)]
MOVES = ([CORE] + ALONG_X + ALONG_Y + ALONG_Z, [CORE] + ALONG_Y + ALONG_X + ALONG_Z)
DUALS = tuple(dual(m) for m in MOVES)


def place_bits(index):
    def bit(mask):
        v = index & mask
        v = v ^ (v >> 4)
        v = v ^ (v >> 2)
        return ((v ^ (v >> 1)) & 1) == 1

    half = bit(DUALS[0][0])
    bits = [half]
    for i in range(1, 5):
        bits.append(jnp.where(half, bit(DUALS[1][i]), bit(DUALS[0][i])))
    return bits


def exchange(value, ids):
    pairs = []
    for index in range(256):
        half = parity(index & DUALS[0][0])
        target = index
        for i in ids:
            target ^= MOVES[half][i]
        pairs.append((index, target))
    return lax.ppermute(value, MESH, pairs)


def pick(chunks, bits, flips):
    if not bits:
        return chunks[0]
    half = len(chunks) // 2
    low = pick(chunks[:half], bits[1:], flips[1:])
    high = pick(chunks[half:], bits[1:], flips[1:])
    return jnp.where(bits[0], low, high) if flips[0] else jnp.where(bits[0], high, low)


SUBSETS = {1: [(1,)], 2: [(1, 1), (0, 1), (1, 0)]}


def named(ids, flips):
    return tuple(i for i, f in zip(ids, flips) if f)


def scatter(value, ids, bits):
    parts = 1 << len(ids)
    rows = value.shape[0] // parts
    chunks = [value[i * rows : (i + 1) * rows] for i in range(parts)]
    mine = [bits[i] for i in ids]
    got = [
        exchange(pick(chunks, mine, flips).astype(bf16), named(ids, flips))
        for flips in SUBSETS[len(ids)]
    ]
    out = pick(chunks, mine, (0,) * len(ids))
    for part in got:
        out = out + part.astype(f32)
    return out


def spread(value, ids):
    if len(ids) == 1:
        return value + exchange(value, ids)
    a, b = ids
    both, second, first = exchange(value, ids), exchange(value, (b,)), exchange(value, (a,))
    return (value + first) + (second + both)


def gather(value, ids, bits):
    got = {(0,) * len(ids): value}
    for flips in SUBSETS[len(ids)]:
        got[flips] = exchange(value, named(ids, flips))
    mine = [bits[i] for i in ids]
    parts = [got[key] for key in sorted(got)]
    return jnp.concatenate([pick(parts, mine, key) for key in sorted(got)])


def sum_everywhere(first, second, scale, bits, pieces):
    half = bits[0]
    value = jnp.where(half, second, first) + exchange(jnp.where(half, first, second), (0,))
    value = scatter(value, (1, 2), bits)
    done = pieces(None, 0)
    value, done = lax.optimization_barrier((value, done))
    value = scatter(value, (3, 4), bits)
    done = pieces(done, 1)
    value, done = lax.optimization_barrier((value, done))
    value = spread(value, (5, 6))
    value = spread(value, (7,))
    value = (value * scale).astype(bf16)
    value = gather(value, (3, 4), bits)
    value = gather(value, (1, 2), bits).reshape(3, 3, C, C)
    other = exchange(value, (0,))
    return (
        jnp.where(half, other, value).astype(f32),
        jnp.where(half, value, other).astype(f32),
        done,
    )


def local(fields, cotangent, w_first, w_second, tile_links):
    count = lax.axis_size("space")
    own = lax.axis_index("space").astype(jnp.int32)
    bits = place_bits(lax.axis_index("dp").astype(jnp.int32) * count + own)
    own, *bits = lax.optimization_barrier((own, *bits))
    own = own.reshape(1)
    partner = [(i, i ^ 1) for i in range(count)]
    neighbour = [(i, (i + 1 if i % 2 else i - 1) % count) for i in range(count)]
    table, near, far, rim, x, cot, w_second = call(
        make_edges_body(count),
        [
            shape((36, 2), jnp.int32),
            shape((T, SEND, C), bf16),
            shape((T, SEND, C), bf16),
            shape((16 * RIM, C), f32),
            shape((T, S, S, C), bf16),
            shape((T, S, S, C), bf16),
            shape((3, 3, C, C), bf16),
        ],
        "shhhh",
        [
            pltpu.VMEM((16 * S, C), f32),
            pltpu.VMEM((16 * 64, C), f32),
            pltpu.VMEM((16 * S, C), f32),
            pltpu.SMEM((T, 4, 5), jnp.int32),
            pltpu.SemaphoreType.DMA((4,)),
        ],
        outs_in="svvvvvv",
    )(
        own,
        *[
            pltpu.with_memory_space_constraint(v, pltpu.HBM)
            for v in (
                tile_links,
                fields.reshape(T, S, S, C),
                cotangent.reshape(T, S, S, C),
                w_second,
            )
        ],
    )
    from_near = lax.ppermute(near, "space", partner)
    from_far = lax.ppermute(far, "space", neighbour)
    interior, padded_x = call(
        conv_back_body,
        [shape((T, PIX, C), f32), shape((T, PAD, C), f32)],
        "vvv",
        [
            pltpu.VMEM((T, PAD, C), f32),
            pltpu.VMEM((T, WIDE, 3 * C), bf16),
            pltpu.VMEM((12 * C, 2 * C), bf16),
        ],
    )(cot, w_second, x)
    active, hidden_grad, wide, act_near, act_far, *_ = call(
        forward_body,
        [
            shape((T, S, S, C), bf16),
            shape((T, PIX, C), bf16),
            shape((T, WIDE, 3 * C), bf16),
            shape((T, S, C), bf16),
            shape((T, S, C), bf16),
            shape((T, PAD, C), f32),
            shape((T, PIX, C), f32),
        ],
        "svvvvvv",
        [
            pltpu.VMEM((24 * S, C), f32),
            pltpu.VMEM((24 * RIM, C), f32),
            pltpu.VMEM((T, PIX, C), f32),
            pltpu.VMEM((T, 4 * S, C), f32),
            pltpu.VMEM((12 * C, 2 * C), bf16),
        ],
        aliases={1: 5, 5: 6},
    )(table, padded_x, from_near, from_far, rim, interior, w_first)
    act_from_near = lax.ppermute(act_near, "space", partner)
    act_from_far = lax.ppermute(act_far, "space", neighbour)
    grad_first, padded_active, turned = call(
        first_grad_body,
        [shape((9 * C, C), f32), shape((T, PAD, C), f32), shape((T, C, PIX), bf16)],
        "vvvv",
        [pltpu.VMEM((C, 9 * C), f32)],
    )(hidden_grad, wide, active, cot)
    grad_second, wide_active, _ = call(
        second_grad_body,
        [shape((9 * C, C), f32), shape((T, WIDE, 3 * C), bf16), shape((T, PAD, C), f32)],
        "svvvv",
        [
            pltpu.VMEM((24 * S, C), f32),
            pltpu.VMEM((C, 9 * C), f32),
        ],
        aliases={1: 2},
    )(table, padded_active, act_from_near, act_from_far, turned)

    def mixed_piece(before, n):
        args = (x, wide_active, w_second) + (() if before is None else (before,))
        (mixed,) = call(
            make_mixed_body(2 * n, 2 * n + 2),
            [shape((T, S, S, C), bf16)],
            "vvvh"[: len(args)],
            [
                pltpu.VMEM((2, S, S, C), bf16),
                pltpu.SemaphoreType.DMA((2,)),
                pltpu.VMEM((12 * C, 2 * C), bf16),
            ],
            outs_in="h",
            aliases={} if before is None else {3: 0},
        )(*args)
        return mixed

    total = lax.axis_size("dp") * count * T * PIX
    first, second, mixed = sum_everywhere(
        grad_first, grad_second, float(total) ** -0.5, bits, mixed_piece
    )
    return (
        mixed.reshape(fields.shape),
        first,
        second,
    )


def solution(mesh):
    placed = (
        P("dp", "space", None, None, None),
        P("dp", "space", None, None, None),
        P(),
        P(),
        P("space", None, None),
    )
    return jax.shard_map(
        local,
        mesh=mesh,
        in_specs=placed,
        out_specs=(P("dp", "space", None, None, None), P(), P()),
        check_vma=False,
    )
```

```python
import jax
import jax.numpy as jnp
from jax import lax
from jax.experimental import pallas as pl
from jax.experimental.pallas import tpu as pltpu
from jax.sharding import PartitionSpec as P

f32 = jnp.float32
bf16 = jnp.bfloat16
S = 32
C = 128
T = 4
PIX = S * S
GAP = 48
LEAD = 8
PAD = (S + 2) * GAP
WIDE = (S + 2) * S
RIM = 48
SEND = S + RIM
MESH = ("dp", "space")


def vmem():
    return pl.BlockSpec(memory_space=pltpu.VMEM)


def smem():
    return pl.BlockSpec(memory_space=pltpu.SMEM)


def hbm():
    return pl.BlockSpec(memory_space=pltpu.HBM)


SPACES = {"s": smem, "v": vmem, "h": hbm}


def call(body, outs, ins, scratch=(), outs_in="", aliases={}, limit=16):
    return pl.pallas_call(
        body,
        out_shape=outs,
        in_specs=[SPACES[k]() for k in ins],
        out_specs=[SPACES[k]() for k in outs_in or "v" * len(outs)],
        scratch_shapes=list(scratch),
        input_output_aliases=aliases,
        compiler_params=pltpu.CompilerParams(vmem_limit_bytes=limit << 20),
    )


def shape(dims, dtype):
    return jax.ShapeDtypeStruct(dims, dtype)


def flip8(block):
    row = lax.broadcasted_iota(jnp.int32, (8, C), 0)
    block = pltpu.roll(block, 4, 0)
    block = jnp.where((row & 2) == 0, pltpu.roll(block, 6, 0), pltpu.roll(block, 2, 0))
    return jnp.where((row & 1) == 0, pltpu.roll(block, 7, 0), pltpu.roll(block, 1, 0))


def flip_line(line):
    parts = [line[8 * i : 8 * i + 8] for i in range(S // 8)]
    return jnp.concatenate([flip8(part) for part in reversed(parts)], axis=0)


def directed(line, flag):
    return jnp.where(jnp.full(line.shape, flag, jnp.int32) == 1, flip_line(line), line)


def link_table(own, links, table, count):
    zero = jnp.int32(0)

    def where_is(source):
        gap = (source >> 2) - own + 1
        gap = jnp.where(gap < 0, gap + count, gap)
        return jnp.where(gap >= count, gap - count, gap), source & 3

    sides = []
    facing = {(way, slot): zero for way in (0, 2) for slot in range(T)}
    for n in range(4 * T):
        rel, slot = where_is(links[n // 4, n % 4, 0])
        edge = links[n // 4, n % 4, 1]
        sides.append((rel, slot, edge))
        for way in (0, 2):
            for s in range(T):
                facing[way, s] += jnp.where((rel == way) & (slot == s), edge, zero)
    odd = (own & 1) == 1
    below = jnp.where(odd, 16, 20)
    above = jnp.where(odd, 20, 16)
    for n, (rel, slot, edge) in enumerate(sides):
        line = jnp.where(rel == 1, slot * 4 + edge, jnp.where(rel == 0, below, above) + slot)
        table[n, 0] = line
        table[n, 1] = links[n // 4, n % 4, 2]
    for n in range(4 * T):
        rel, slot = where_is(links[n // 4, n % 4, 3])
        at = links[n // 4, n % 4, 4]
        low, high = zero, zero
        for s in range(T):
            low += jnp.where(slot == s, facing[0, s], zero)
            high += jnp.where(slot == s, facing[2, s], zero)
        face = jnp.where(rel == 0, low, high)
        start = jnp.where(face == 1, 1, jnp.where(face == 2, 3, 0))
        near = slot * 4 + jnp.where(at < 2, 0, 2)
        line = jnp.where(rel == 1, near, jnp.where(rel == 0, below, above) + slot)
        far_end = jnp.where(at == start, 0, 1)
        near_end = jnp.where((at == 1) | (at == 2), 1, 0)
        table[16 + n, 0] = line
        table[16 + n, 1] = jnp.where(rel == 1, near_end, far_end)
    faces = []
    for t in range(T):
        low, high = zero, zero
        for k in range(4):
            rel = sides[t * 4 + k][0]
            low += jnp.where(rel == 0, k, 0)
            high += jnp.where(rel == 2, k, 0)
        low, high = jnp.where(odd, low, high), jnp.where(odd, high, low)
        table[32 + t, 0] = low
        table[32 + t, 1] = high
        faces.append((low, high))
    return faces


def make_edges_body(count):
    def body(
        own, tile_links, fields_far, cot_far, w_second_far, w_first_far,
        table, near, far, rim, fields, cot, w_second, w_first,
        lines, wide, slab, links, sems,
    ):
        copies = [
            pltpu.make_async_copy(source, target, sems.at[n])
            for n, (source, target) in enumerate(
                (
                    (tile_links, links),
                    (cot_far, cot),
                    (w_second_far, w_second),
                    (fields_far, fields),
                    (w_first_far, w_first),
                )
            )
        ]
        for copy in copies:
            copy.start()
        wide[...] = jnp.zeros(wide.shape, f32)
        copies[0].wait()
        faces = link_table(own[0], links, table, count)

        def put_lines(source, t, store):
            store(0, source[t, 0].astype(f32))
            store(2, source[t, S - 1].astype(f32))
            for edge, first, at in ((3, 0, 0), (1, 16, 15)):
                slab[...] = source[t, :, first : first + 16, :].astype(f32).reshape(16 * S, C)
                store(edge, slab[pl.ds(at, S, stride=16), :])

        copies[1].wait()
        for t in range(T):

            def store(k, line, t=t):
                wide[(k * T + t) * 64 + 16 : (k * T + t) * 64 + 16 + S, :] = line

            put_lines(cot, t, store)
        taps = {
            0: [(0, c) for c in range(3)],
            1: [(r, 2) for r in range(3)],
            2: [(2, c) for c in range(3)],
            3: [(r, 0) for r in range(3)],
        }
        copies[2].wait()
        for k in range(4):
            left = []
            for t in range(T):
                base = (k * T + t) * 64
                left.append(
                    jnp.concatenate(
                        [wide[base + 9 - c : base + 9 - c + RIM, :].astype(bf16) for c in range(3)],
                        axis=1,
                    )
                )
            left = jnp.concatenate(left, axis=0)
            right = jnp.concatenate([w_second[r, c] for r, c in taps[k]], axis=1)
            out = lax.dot_general(
                left, right, (((1,), (1,)), ((), ())), preferred_element_type=f32
            )
            for t in range(T):
                rim[(t * 4 + k) * RIM : (t * 4 + k + 1) * RIM, :] = out[t * RIM : (t + 1) * RIM]
        copies[3].wait()
        copies[4].wait()
        for t in range(T):

            def store(k, line, t=t):
                lines[(t * 4 + k) * S : (t * 4 + k + 1) * S, :] = line

            put_lines(fields, t, store)
        for t in range(T):
            for out_ref, face in zip((near, far), faces[t]):
                n = t * 4 + face
                at = pl.multiple_of(n * S, S)
                out_ref[t, 0:S, :] = lines[pl.ds(at, S), :].astype(bf16)
                at = pl.multiple_of(n * RIM, 16)
                out_ref[t, S:SEND, :] = rim[pl.ds(at, RIM), :].astype(bf16)

    return body


def widen(padded, t, wide):
    for p in range(S + 2):
        for c in range(3):
            at = p * GAP + LEAD - 1 + c
            wide[t, p * S : (p + 1) * S, c * C : (c + 1) * C] = padded[t, at : at + S, :].astype(bf16)


def taps_of(wide, t, first, rows):
    return jnp.concatenate(
        [wide[t, r * S + first : r * S + first + rows, :] for r in range(3)], axis=1
    )


def pair_taps(wide, t, first, pairs):
    parts = []
    for r in range(4):
        parts.append(
            jnp.concatenate(
                [wide[t, (2 * p + r) * S : (2 * p + r + 1) * S, :] for p in range(first, first + pairs)],
                axis=0,
            )
        )
    return jnp.concatenate(parts, axis=1)


def pair_kernel(tap):
    zero = jnp.zeros((C, C), bf16)
    rows = []
    for r in range(4):
        for c in range(3):
            even = tap(r, c) if r < 3 else zero
            odd = tap(r - 1, c) if r > 0 else zero
            rows.append(jnp.concatenate([even, odd], axis=1))
    return jnp.concatenate(rows, axis=0)


def pair_conv(wide, t, first, pairs, right):
    got = jnp.dot(pair_taps(wide, t, first, pairs), right, preferred_element_type=f32)
    for p in range(pairs):
        for odd in range(2):
            yield 2 * (first + p) + odd, got[p * S : (p + 1) * S, odd * C : (odd + 1) * C]


def put_interior(source, padded, t):
    for r in range(S):
        at = (1 + r) * GAP + LEAD
        padded[t, at : at + S, :] = source[t, r].astype(f32)


def conv_back_body(
    cot, w_second, fields, w_first, out, padded_fields, first_right, padded, wide, right
):
    first_right[...] = pair_kernel(lambda r, c: w_first[r, c])
    for t in range(T):
        put_interior(fields, padded_fields, t)
    right[...] = pair_kernel(lambda r, c: w_second[2 - r, 2 - c].T)
    zero = jnp.zeros((GAP, C), f32)
    for t in range(T):
        padded[t, 0:GAP, :] = zero
        padded[t, PAD - GAP : PAD, :] = zero
        for r in range(S):
            at = (1 + r) * GAP
            padded[t, at : at + 8, :] = zero[:8]
            padded[t, at + LEAD + S : at + GAP, :] = zero[:8]
        put_interior(cot, padded, t)
        widen(padded, t, wide)
        for first in range(0, S // 2, 8):
            for row, value in pair_conv(wide, t, first, 8, right[...]):
                out[t, row * S : (row + 1) * S, :] = value


def collect_lines(padded, lines, near, far):
    for t in range(T):
        base = GAP + LEAD
        spots = {
            0: padded[t, base : base + S, :],
            1: padded[t, pl.ds(base + S - 1, S, stride=GAP), :],
            2: padded[t, base + (S - 1) * GAP : base + (S - 1) * GAP + S, :],
            3: padded[t, pl.ds(base, S, stride=GAP), :],
        }
        for k in range(4):
            lines[(t * 4 + k) * S : (t * 4 + k + 1) * S, :] = spots[k]
        for first, received in ((16, near), (20, far)):
            lines[(first + t) * S : (first + t + 1) * S, :] = received[t, 0:S, :].astype(f32)


def put_rims(table, lines, padded):
    for t in range(T):
        for k in range(4):
            n = t * 4 + k
            at = pl.multiple_of(table[n, 0] * S, S)
            line = directed(lines[pl.ds(at, S), :], table[n, 1])
            if k == 0:
                padded[t, LEAD : LEAD + S, :] = line
            elif k == 2:
                at = (S + 1) * GAP + LEAD
                padded[t, at : at + S, :] = line
            elif k == 1:
                padded[t, pl.ds(GAP + LEAD + S, S, stride=GAP), :] = line
            else:
                padded[t, pl.ds(GAP + LEAD - 1, S, stride=GAP), :] = line
        for k, spot in enumerate(
            (
                LEAD - 1,
                LEAD + S,
                (S + 1) * GAP + LEAD + S,
                (S + 1) * GAP + LEAD - 1,
            )
        ):
            n = 16 + t * 4 + k
            at = table[n, 0] * S + table[n, 1] * (S - 1)
            padded[t, spot : spot + 1, :] = lines[pl.ds(at, 1), :]


def forward_body(
    table, padded_in, near, far, rim, interior, right,
    active, hidden_grad, wide, send_near, send_far, padded, grads,
    lines, rims, rounded, edges,
):
    collect_lines(padded, lines, near, far)
    put_rims(table, lines, padded)
    rims[0 : 16 * RIM, :] = rim[...]
    for t in range(T):
        rims[(16 + t) * RIM : (17 + t) * RIM, :] = near[t, S:SEND, :].astype(f32)
        rims[(20 + t) * RIM : (21 + t) * RIM, :] = far[t, S:SEND, :].astype(f32)
    for t in range(T):
        for k in range(4):
            n = t * 4 + k
            at = pl.multiple_of(table[n, 0] * RIM, 16)
            line = directed(rims[pl.ds(at + 8, S), :], table[n, 1])
            if k == 0:
                grads[t, 0:S, :] += line
            elif k == 2:
                grads[t, PIX - S : PIX, :] += line
            else:
                spot = pl.ds(S - 1 if k == 1 else 0, S, stride=S)
                grads[t, spot, :] = grads[t, spot, :] + line
        for k, spot in enumerate((0, S - 1, PIX - 1, PIX - S)):
            n = 16 + t * 4 + k
            at = table[n, 0] * RIM + 7 + table[n, 1] * (S + 1)
            grads[t, spot : spot + 1, :] += rims[pl.ds(at, 1), :]
    for t in range(T):
        widen(padded, t, wide)
        for first in range(0, S // 2, 8):
            for row, hidden in pair_conv(wide, t, first, 8, right[...]):
                gate = 1.0 / (1.0 + jnp.exp(-hidden))
                act = (hidden * gate).astype(bf16)
                active[t, row] = act
                span = slice(row * S, (row + 1) * S)
                rounded[t, span, :] = act.astype(f32)
                hidden_grad[t, span, :] = (
                    grads[t, span, :] * gate * (1.0 + hidden * (1.0 - gate))
                ).astype(bf16)
    for t in range(T):
        edges[t, 0:S, :] = rounded[t, 0:S, :]
        edges[t, S : 2 * S, :] = rounded[t, pl.ds(S - 1, S, stride=S), :]
        edges[t, 2 * S : 3 * S, :] = rounded[t, PIX - S : PIX, :]
        edges[t, 3 * S : 4 * S, :] = rounded[t, pl.ds(0, S, stride=S), :]
        for out_ref, which in ((send_near, 0), (send_far, 1)):
            at = pl.multiple_of(table[32 + t, which] * S, S)
            out_ref[t] = edges[t, pl.ds(at, S), :].astype(bf16)


def weight_grad(cot_of, wide, acc, out):
    for t in range(T):
        got = jnp.dot(
            cot_of(t),
            jnp.concatenate([wide[t, r * S : r * S + PIX, :] for r in range(3)], axis=1),
            preferred_element_type=f32,
        )
        acc[...] = got if t == 0 else acc[...] + got
    for n in range(9):
        out[n * C : (n + 1) * C, :] = acc[:, n * C : (n + 1) * C].T


def first_grad_body(
    hidden_grad, wide, active, cot, w_second, out, padded, turned, second_right, acc
):
    weight_grad(lambda t: hidden_grad[t].T, wide, acc, out)
    for t in range(T):
        put_interior(active, padded, t)
        turned[t] = cot[t].reshape(PIX, C).T
    second_right[...] = pair_kernel(lambda r, c: w_second[r, c])


def second_grad_body(table, padded_in, near, far, turned, out, wide, padded, lines, acc):
    collect_lines(padded, lines, near, far)
    put_rims(table, lines, padded)
    for t in range(T):
        widen(padded, t, wide)
    weight_grad(lambda t: turned[t], wide, acc, out)


def mix_tile(fields, wide, right, t, tile):
    for first in range(0, S // 2, 8):
        for row, value in pair_conv(wide, t, first, 8, right[...]):
            tile[row] = (fields[t, row].astype(f32) + value).astype(bf16)


def make_mixed_body(t):
    def body(fields, wide, right, tile):
        mix_tile(fields, wide, right, t, tile)

    return body


def last_mixed_body(fields, wide, right, first, second, third, out, tile, sems):
    copies = [
        pltpu.make_async_copy(source, out.at[t], sems.at[t])
        for t, source in enumerate((first, second, third, tile))
    ]
    for copy in copies[:3]:
        copy.start()
    mix_tile(fields, wide, right, 3, tile)
    copies[3].start()
    for copy in copies:
        copy.wait()


def move(x=0, y=0, z=0):
    return 1 | (y << 1) | ((z >> 1) << 3) | (x << 5) | ((z & 1) << 7)


def parity(value):
    return bin(value).count("1") & 1


def dual(basis):
    size = len(basis)
    rows = [[(m >> k) & 1 for k in range(size)] + [int(k == i) for k in range(size)] for i, m in enumerate(basis)]
    for c in range(size):
        pivot = next(r for r in range(c, size) if rows[r][c])
        rows[c], rows[pivot] = rows[pivot], rows[c]
        for r in range(size):
            if r != c and rows[r][c]:
                rows[r] = [p ^ q for p, q in zip(rows[r], rows[c])]
    return [sum(rows[k][size + i] << k for k in range(size)) for i in range(size)]


CORE = 1
ALONG_X = [move(x=1), move(x=3)]
ALONG_Y = [move(y=1), move(y=3)]
ALONG_Z = [move(z=1), move(z=2), move(z=7)]
MOVES = ([CORE] + ALONG_X + ALONG_Y + ALONG_Z, [CORE] + ALONG_Y + ALONG_X + ALONG_Z)
DUALS = tuple(dual(m) for m in MOVES)


def place_bits(index):
    def bit(mask):
        v = index & mask
        v = v ^ (v >> 4)
        v = v ^ (v >> 2)
        return ((v ^ (v >> 1)) & 1) == 1

    half = bit(DUALS[0][0])
    bits = [half]
    for i in range(1, 5):
        bits.append(jnp.where(half, bit(DUALS[1][i]), bit(DUALS[0][i])))
    return bits


def exchange(value, ids):
    pairs = []
    for index in range(256):
        half = parity(index & DUALS[0][0])
        target = index
        for i in ids:
            target ^= MOVES[half][i]
        pairs.append((index, target))
    return lax.ppermute(value, MESH, pairs)


def pick(chunks, bits, flips):
    if not bits:
        return chunks[0]
    half = len(chunks) // 2
    low = pick(chunks[:half], bits[1:], flips[1:])
    high = pick(chunks[half:], bits[1:], flips[1:])
    return jnp.where(bits[0], low, high) if flips[0] else jnp.where(bits[0], high, low)


SUBSETS = {1: [(1,)], 2: [(1, 1), (0, 1), (1, 0)]}


def named(ids, flips):
    return tuple(i for i, f in zip(ids, flips) if f)


def scatter(value, ids, bits):
    parts = 1 << len(ids)
    rows = value.shape[0] // parts
    chunks = [value[i * rows : (i + 1) * rows] for i in range(parts)]
    mine = [bits[i] for i in ids]
    got = [
        exchange(pick(chunks, mine, flips).astype(bf16), named(ids, flips))
        for flips in SUBSETS[len(ids)]
    ]
    out = pick(chunks, mine, (0,) * len(ids))
    for part in got:
        out = out + part.astype(f32)
    return out


def spread(value, ids, bits):
    if len(ids) == 1:
        return value + exchange(value, ids)
    a, b = ids
    both, second, first = exchange(value, ids), exchange(value, (b,)), exchange(value, (a,))
    return (value + first) + (second + both)


def gather(value, ids, bits):
    got = {(0,) * len(ids): value}
    for flips in SUBSETS[len(ids)]:
        got[flips] = exchange(value, named(ids, flips))
    mine = [bits[i] for i in ids]
    parts = [got[key] for key in sorted(got)]
    return jnp.concatenate([pick(parts, mine, key) for key in sorted(got)])


def sum_everywhere(first, second, scale, bits, pieces):
    half = bits[0]
    value = jnp.where(half, second, first) + exchange(jnp.where(half, first, second), (0,))
    tiles = []
    for step, ids in ((scatter, (1, 2)), (scatter, (3, 4)), (spread, (5, 6)), (spread, (7,))):
        value = step(value, ids, bits)
        value, tile = lax.optimization_barrier((value, pieces(tiles)))
        tiles.append(tile)
    value = (value * scale).astype(bf16)
    value = gather(value, (3, 4), bits)
    value = gather(value, (1, 2), bits).reshape(3, 3, C, C)
    other = exchange(value, (0,))
    return (
        jnp.where(half, other, value).astype(f32),
        jnp.where(half, value, other).astype(f32),
        tiles[-1],
    )


def local(fields, cotangent, w_first, w_second, tile_links):
    count = lax.axis_size("space")
    own = lax.axis_index("space").astype(jnp.int32)
    bits = place_bits(lax.axis_index("dp").astype(jnp.int32) * count + own)
    own, *bits = lax.optimization_barrier((own, *bits))
    own = own.reshape(1)
    partner = [(i, i ^ 1) for i in range(count)]
    neighbour = [(i, (i + 1 if i % 2 else i - 1) % count) for i in range(count)]
    table, near, far, rim, x, cot, w_second, w_first = call(
        make_edges_body(count),
        [
            shape((36, 2), jnp.int32),
            shape((T, SEND, C), bf16),
            shape((T, SEND, C), bf16),
            shape((16 * RIM, C), f32),
            shape((T, S, S, C), bf16),
            shape((T, S, S, C), bf16),
            shape((3, 3, C, C), bf16),
            shape((3, 3, C, C), bf16),
        ],
        "shhhhh",
        [
            pltpu.VMEM((16 * S, C), f32),
            pltpu.VMEM((16 * 64, C), f32),
            pltpu.VMEM((16 * S, C), f32),
            pltpu.SMEM((T, 4, 5), jnp.int32),
            pltpu.SemaphoreType.DMA((5,)),
        ],
        outs_in="svvvvvvv",
    )(
        own,
        *[
            pltpu.with_memory_space_constraint(v, pltpu.HBM)
            for v in (
                tile_links,
                fields.reshape(T, S, S, C),
                cotangent.reshape(T, S, S, C),
                w_second,
                w_first,
            )
        ],
    )
    from_near = lax.ppermute(near, "space", partner)
    from_far = lax.ppermute(far, "space", neighbour)
    interior, padded_x, first_right = call(
        conv_back_body,
        [shape((T, PIX, C), f32), shape((T, PAD, C), f32), shape((12 * C, 2 * C), bf16)],
        "vvvv",
        [
            pltpu.VMEM((T, PAD, C), f32),
            pltpu.VMEM((T, WIDE, 3 * C), bf16),
            pltpu.VMEM((12 * C, 2 * C), bf16),
        ],
    )(cot, w_second, x, w_first)
    active, hidden_grad, wide, act_near, act_far, *_ = call(
        forward_body,
        [
            shape((T, S, S, C), bf16),
            shape((T, PIX, C), bf16),
            shape((T, WIDE, 3 * C), bf16),
            shape((T, S, C), bf16),
            shape((T, S, C), bf16),
            shape((T, PAD, C), f32),
            shape((T, PIX, C), f32),
        ],
        "svvvvvv",
        [
            pltpu.VMEM((24 * S, C), f32),
            pltpu.VMEM((24 * RIM, C), f32),
            pltpu.VMEM((T, PIX, C), f32),
            pltpu.VMEM((T, 4 * S, C), f32),
        ],
        aliases={1: 5, 5: 6},
    )(table, padded_x, from_near, from_far, rim, interior, first_right)
    act_from_near = lax.ppermute(act_near, "space", partner)
    act_from_far = lax.ppermute(act_far, "space", neighbour)
    grad_first, padded_active, turned, second_right = call(
        first_grad_body,
        [
            shape((9 * C, C), f32),
            shape((T, PAD, C), f32),
            shape((T, C, PIX), bf16),
            shape((12 * C, 2 * C), bf16),
        ],
        "vvvvv",
        [pltpu.VMEM((C, 9 * C), f32)],
    )(hidden_grad, wide, active, cot, w_second)
    grad_second, wide_active, _ = call(
        second_grad_body,
        [shape((9 * C, C), f32), shape((T, WIDE, 3 * C), bf16), shape((T, PAD, C), f32)],
        "svvvv",
        [
            pltpu.VMEM((24 * S, C), f32),
            pltpu.VMEM((C, 9 * C), f32),
        ],
        aliases={1: 2},
    )(table, padded_active, act_from_near, act_from_far, turned)

    def mixed_piece(tiles):
        t = len(tiles)
        if t < T - 1:
            (tile,) = call(make_mixed_body(t), [shape((S, S, C), bf16)], "vvv")(
                x, wide_active, second_right
            )
            return tile
        (mixed,) = call(
            last_mixed_body,
            [shape((T, S, S, C), bf16)],
            "vvvvvv",
            [pltpu.VMEM((S, S, C), bf16), pltpu.SemaphoreType.DMA((T,))],
            outs_in="h",
        )(x, wide_active, second_right, *tiles)
        return mixed

    total = lax.axis_size("dp") * count * T * PIX
    first, second, mixed = sum_everywhere(
        grad_first, grad_second, float(total) ** -0.5, bits, mixed_piece
    )
    return (
        mixed.reshape(fields.shape),
        first,
        second,
    )


def solution(mesh):
    placed = (
        P("dp", "space", None, None, None),
        P("dp", "space", None, None, None),
        P(),
        P(),
        P("space", None, None),
    )
    return jax.shard_map(
        local,
        mesh=mesh,
        in_specs=placed,
        out_specs=(P("dp", "space", None, None, None), P(), P()),
        check_vma=False,
    )
```

```python
import jax
import jax.numpy as jnp
from jax import lax
from jax.experimental import pallas as pl
from jax.experimental.pallas import tpu as pltpu
from jax.sharding import PartitionSpec as P

f32 = jnp.float32
bf16 = jnp.bfloat16
S = 32
C = 128
T = 4
PIX = S * S
GAP = 48
LEAD = 8
PAD = (S + 2) * GAP
WIDE = (S + 2) * S
RIM = 48
SEND = S + RIM
MESH = ("dp", "space")


def vmem():
    return pl.BlockSpec(memory_space=pltpu.VMEM)


def smem():
    return pl.BlockSpec(memory_space=pltpu.SMEM)


def hbm():
    return pl.BlockSpec(memory_space=pltpu.HBM)


SPACES = {"s": smem, "v": vmem, "h": hbm}


def call(body, outs, ins, scratch=(), outs_in="", aliases={}, limit=16):
    return pl.pallas_call(
        body,
        out_shape=outs,
        in_specs=[SPACES[k]() for k in ins],
        out_specs=[SPACES[k]() for k in outs_in or "v" * len(outs)],
        scratch_shapes=list(scratch),
        input_output_aliases=aliases,
        compiler_params=pltpu.CompilerParams(vmem_limit_bytes=limit << 20),
    )


def shape(dims, dtype):
    return jax.ShapeDtypeStruct(dims, dtype)


def flip8(block):
    row = lax.broadcasted_iota(jnp.int32, (8, C), 0)
    block = pltpu.roll(block, 4, 0)
    block = jnp.where((row & 2) == 0, pltpu.roll(block, 6, 0), pltpu.roll(block, 2, 0))
    return jnp.where((row & 1) == 0, pltpu.roll(block, 7, 0), pltpu.roll(block, 1, 0))


def flip_line(line):
    parts = [line[8 * i : 8 * i + 8] for i in range(S // 8)]
    return jnp.concatenate([flip8(part) for part in reversed(parts)], axis=0)


def directed(line, flag):
    return jnp.where(jnp.full(line.shape, flag, jnp.int32) == 1, flip_line(line), line)


def link_table(own, links, table, count):
    zero = jnp.int32(0)

    def where_is(source):
        gap = (source >> 2) - own + 1
        gap = jnp.where(gap < 0, gap + count, gap)
        return jnp.where(gap >= count, gap - count, gap), source & 3

    sides = []
    facing = {(way, slot): zero for way in (0, 2) for slot in range(T)}
    for n in range(4 * T):
        rel, slot = where_is(links[n // 4, n % 4, 0])
        edge = links[n // 4, n % 4, 1]
        sides.append((rel, slot, edge))
        for way in (0, 2):
            for s in range(T):
                facing[way, s] += jnp.where((rel == way) & (slot == s), edge, zero)
    odd = (own & 1) == 1
    below = jnp.where(odd, 16, 20)
    above = jnp.where(odd, 20, 16)
    for n, (rel, slot, edge) in enumerate(sides):
        line = jnp.where(rel == 1, slot * 4 + edge, jnp.where(rel == 0, below, above) + slot)
        table[n, 0] = line
        table[n, 1] = links[n // 4, n % 4, 2]
    for n in range(4 * T):
        rel, slot = where_is(links[n // 4, n % 4, 3])
        at = links[n // 4, n % 4, 4]
        low, high = zero, zero
        for s in range(T):
            low += jnp.where(slot == s, facing[0, s], zero)
            high += jnp.where(slot == s, facing[2, s], zero)
        face = jnp.where(rel == 0, low, high)
        start = jnp.where(face == 1, 1, jnp.where(face == 2, 3, 0))
        near = slot * 4 + jnp.where(at < 2, 0, 2)
        line = jnp.where(rel == 1, near, jnp.where(rel == 0, below, above) + slot)
        far_end = jnp.where(at == start, 0, 1)
        near_end = jnp.where((at == 1) | (at == 2), 1, 0)
        table[16 + n, 0] = line
        table[16 + n, 1] = jnp.where(rel == 1, near_end, far_end)
    faces = []
    for t in range(T):
        low, high = zero, zero
        for k in range(4):
            rel = sides[t * 4 + k][0]
            low += jnp.where(rel == 0, k, 0)
            high += jnp.where(rel == 2, k, 0)
        low, high = jnp.where(odd, low, high), jnp.where(odd, high, low)
        table[32 + t, 0] = low
        table[32 + t, 1] = high
        faces.append((low, high))
    return faces


def make_edges_body(count):
    def body(
        own, tile_links, fields_far, cot_far, w_second_far, w_first_far,
        table, near, far, rim, fields, cot, w_second, w_first, cot_lines,
        lines, wide, slab, links, sems,
    ):
        copies = [
            pltpu.make_async_copy(source, target, sems.at[n])
            for n, (source, target) in enumerate(
                (
                    (tile_links, links),
                    (cot_far, cot),
                    (w_second_far, w_second),
                    (fields_far, fields),
                    (w_first_far, w_first),
                )
            )
        ]
        for copy in copies:
            copy.start()
        wide[...] = jnp.zeros(wide.shape, f32)
        copies[0].wait()
        faces = link_table(own[0], links, table, count)

        def put_lines(source, t, store):
            store(0, source[t, 0].astype(f32))
            store(2, source[t, S - 1].astype(f32))
            for edge, first, at in ((3, 0, 0), (1, 16, 15)):
                slab[...] = source[t, :, first : first + 16, :].astype(f32).reshape(16 * S, C)
                store(edge, slab[pl.ds(at, S, stride=16), :])

        copies[1].wait()
        for t in range(T):

            def store(k, line, t=t):
                wide[(k * T + t) * 64 + 16 : (k * T + t) * 64 + 16 + S, :] = line
                cot_lines[k, t * S : (t + 1) * S, :] = line

            put_lines(cot, t, store)
        taps = {
            0: [(0, c) for c in range(3)],
            1: [(r, 2) for r in range(3)],
            2: [(2, c) for c in range(3)],
            3: [(r, 0) for r in range(3)],
        }
        copies[2].wait()
        for k in range(4):
            left = []
            for t in range(T):
                base = (k * T + t) * 64
                left.append(
                    jnp.concatenate(
                        [wide[base + 9 - c : base + 9 - c + RIM, :].astype(bf16) for c in range(3)],
                        axis=1,
                    )
                )
            left = jnp.concatenate(left, axis=0)
            right = jnp.concatenate([w_second[r, c] for r, c in taps[k]], axis=1)
            out = lax.dot_general(
                left, right, (((1,), (1,)), ((), ())), preferred_element_type=f32
            )
            for t in range(T):
                rim[(t * 4 + k) * RIM : (t * 4 + k + 1) * RIM, :] = out[t * RIM : (t + 1) * RIM]
        copies[3].wait()
        copies[4].wait()
        for t in range(T):

            def store(k, line, t=t):
                lines[(t * 4 + k) * S : (t * 4 + k + 1) * S, :] = line

            put_lines(fields, t, store)
        for t in range(T):
            for out_ref, face in zip((near, far), faces[t]):
                n = t * 4 + face
                at = pl.multiple_of(n * S, S)
                out_ref[t, 0:S, :] = lines[pl.ds(at, S), :].astype(bf16)
                at = pl.multiple_of(n * RIM, 16)
                out_ref[t, S:SEND, :] = rim[pl.ds(at, RIM), :].astype(bf16)

    return body


def widen(padded, t, wide):
    for p in range(S + 2):
        for c in range(3):
            at = p * GAP + LEAD - 1 + c
            wide[t, p * S : (p + 1) * S, c * C : (c + 1) * C] = padded[t, at : at + S, :].astype(bf16)


def pair_taps(wide, t, first, pairs):
    parts = []
    for r in range(4):
        parts.append(
            jnp.concatenate(
                [wide[t, (2 * p + r) * S : (2 * p + r + 1) * S, :] for p in range(first, first + pairs)],
                axis=0,
            )
        )
    return jnp.concatenate(parts, axis=1)


def pair_kernel(tap):
    zero = jnp.zeros((C, C), bf16)
    rows = []
    for r in range(4):
        for c in range(3):
            even = tap(r, c) if r < 3 else zero
            odd = tap(r - 1, c) if r > 0 else zero
            rows.append(jnp.concatenate([even, odd], axis=1))
    return jnp.concatenate(rows, axis=0)


def pair_conv(wide, t, first, pairs, right):
    got = jnp.dot(pair_taps(wide, t, first, pairs), right, preferred_element_type=f32)
    for p in range(pairs):
        for odd in range(2):
            yield 2 * (first + p) + odd, got[p * S : (p + 1) * S, odd * C : (odd + 1) * C]


def put_interior(source, padded, t):
    for r in range(S):
        at = (1 + r) * GAP + LEAD
        padded[t, at : at + S, :] = source[t, r].astype(f32)


def clear_rims(padded, t):
    zero = jnp.zeros((GAP, C), f32)
    padded[t, 0:GAP, :] = zero
    padded[t, PAD - GAP : PAD, :] = zero
    for r in range(S):
        at = (1 + r) * GAP
        padded[t, at : at + 8, :] = zero[:8]
        padded[t, at + LEAD + S : at + GAP, :] = zero[:8]


def conv_back_body(
    cot, w_second, fields, w_first, out, padded_fields, first_right, padded, wide, right
):
    first_right[...] = pair_kernel(lambda r, c: w_first[r, c])
    for t in range(T):
        put_interior(fields, padded_fields, t)
    right[...] = pair_kernel(lambda r, c: w_second[2 - r, 2 - c].T)
    for t in range(T):
        clear_rims(padded, t)
        put_interior(cot, padded, t)
        widen(padded, t, wide)
        for first in range(0, S // 2, 8):
            for row, value in pair_conv(wide, t, first, 8, right[...]):
                out[t, row * S : (row + 1) * S, :] = value


def collect_lines(padded, lines, near, far):
    for t in range(T):
        base = GAP + LEAD
        spots = {
            0: padded[t, base : base + S, :],
            1: padded[t, pl.ds(base + S - 1, S, stride=GAP), :],
            2: padded[t, base + (S - 1) * GAP : base + (S - 1) * GAP + S, :],
            3: padded[t, pl.ds(base, S, stride=GAP), :],
        }
        for k in range(4):
            lines[(t * 4 + k) * S : (t * 4 + k + 1) * S, :] = spots[k]
        for first, received in ((16, near), (20, far)):
            lines[(first + t) * S : (first + t + 1) * S, :] = received[t, 0:S, :].astype(f32)


def put_rims(table, lines, padded):
    for t in range(T):
        for k in range(4):
            n = t * 4 + k
            at = pl.multiple_of(table[n, 0] * S, S)
            line = directed(lines[pl.ds(at, S), :], table[n, 1])
            if k == 0:
                padded[t, LEAD : LEAD + S, :] = line
            elif k == 2:
                at = (S + 1) * GAP + LEAD
                padded[t, at : at + S, :] = line
            elif k == 1:
                padded[t, pl.ds(GAP + LEAD + S, S, stride=GAP), :] = line
            else:
                padded[t, pl.ds(GAP + LEAD - 1, S, stride=GAP), :] = line
        for k, spot in enumerate(
            (
                LEAD - 1,
                LEAD + S,
                (S + 1) * GAP + LEAD + S,
                (S + 1) * GAP + LEAD - 1,
            )
        ):
            n = 16 + t * 4 + k
            at = table[n, 0] * S + table[n, 1] * (S - 1)
            padded[t, spot : spot + 1, :] = lines[pl.ds(at, 1), :]


def forward_body(
    table, padded_in, near, far, rim, interior, right,
    active, hidden_grad, wide, send_near, send_far, padded, grads,
    lines, rims, rounded, edges,
):
    collect_lines(padded, lines, near, far)
    put_rims(table, lines, padded)
    rims[0 : 16 * RIM, :] = rim[...]
    for t in range(T):
        rims[(16 + t) * RIM : (17 + t) * RIM, :] = near[t, S:SEND, :].astype(f32)
        rims[(20 + t) * RIM : (21 + t) * RIM, :] = far[t, S:SEND, :].astype(f32)
    for t in range(T):
        for k in range(4):
            n = t * 4 + k
            at = pl.multiple_of(table[n, 0] * RIM, 16)
            line = directed(rims[pl.ds(at + 8, S), :], table[n, 1])
            if k == 0:
                grads[t, 0:S, :] += line
            elif k == 2:
                grads[t, PIX - S : PIX, :] += line
            else:
                spot = pl.ds(S - 1 if k == 1 else 0, S, stride=S)
                grads[t, spot, :] = grads[t, spot, :] + line
        for k, spot in enumerate((0, S - 1, PIX - 1, PIX - S)):
            n = 16 + t * 4 + k
            at = table[n, 0] * RIM + 7 + table[n, 1] * (S + 1)
            grads[t, spot : spot + 1, :] += rims[pl.ds(at, 1), :]
    for t in range(T):
        widen(padded, t, wide)
        for first in range(0, S // 2, 8):
            for row, hidden in pair_conv(wide, t, first, 8, right[...]):
                gate = 1.0 / (1.0 + jnp.exp(-hidden))
                act = (hidden * gate).astype(bf16)
                active[t, row] = act
                span = slice(row * S, (row + 1) * S)
                rounded[t, span, :] = act.astype(f32)
                hidden_grad[t, span, :] = (
                    grads[t, span, :] * gate * (1.0 + hidden * (1.0 - gate))
                ).astype(bf16)
    for t in range(T):
        edges[t, 0:S, :] = rounded[t, 0:S, :]
        edges[t, S : 2 * S, :] = rounded[t, pl.ds(S - 1, S, stride=S), :]
        edges[t, 2 * S : 3 * S, :] = rounded[t, PIX - S : PIX, :]
        edges[t, 3 * S : 4 * S, :] = rounded[t, pl.ds(0, S, stride=S), :]
        for out_ref, which in ((send_near, 0), (send_far, 1)):
            at = pl.multiple_of(table[32 + t, which] * S, S)
            out_ref[t] = edges[t, pl.ds(at, S), :].astype(bf16)


def weight_grad(left_of, wide, acc):
    for t in range(T):
        got = jnp.dot(
            left_of(t),
            jnp.concatenate([wide[t, r * S : r * S + PIX, :] for r in range(3)], axis=1),
            preferred_element_type=f32,
        )
        acc[...] = got if t == 0 else acc[...] + got


def put_blocks(acc, out):
    for n in range(9):
        out[n * C : (n + 1) * C, :] = acc[:, n * C : (n + 1) * C].T


def first_grad_body(
    hidden_grad, wide, active, cot, w_second, cot_lines,
    out, padded, inner, turned_lines, second_right, acc, wide_active,
):
    weight_grad(lambda t: hidden_grad[t].T, wide, acc)
    put_blocks(acc, out)
    for t in range(T):
        clear_rims(padded, t)
        put_interior(active, padded, t)
        widen(padded, t, wide_active)
    weight_grad(lambda t: cot[t].reshape(PIX, C).T, wide_active, inner)
    for k in range(4):
        turned_lines[k] = cot_lines[k].T.astype(bf16)
    second_right[...] = pair_kernel(lambda r, c: w_second[r, c])


def second_grad_body(table, padded_in, near, far, inner, turned_lines, out, padded, lines, acc):
    collect_lines(padded, lines, near, far)
    put_rims(table, lines, padded)
    acc[...] = inner[...]
    step = lax.broadcasted_iota(jnp.int32, (S, C), 0)
    for k in range(4):
        rows = []
        for t in range(T):
            taps = []
            for n in range(3):
                if k == 0:
                    tap = padded[t, LEAD - 1 + n : LEAD - 1 + n + S, :]
                elif k == 2:
                    at = (S + 1) * GAP + LEAD - 1 + n
                    tap = padded[t, at : at + S, :]
                else:
                    at = n * GAP + (LEAD + S if k == 1 else LEAD - 1)
                    tap = padded[t, pl.ds(at, S, stride=GAP), :]
                    if n == 0:
                        tap = jnp.where(step == 0, 0.0, tap)
                    elif n == 2:
                        tap = jnp.where(step == S - 1, 0.0, tap)
                taps.append(tap.astype(bf16))
            rows.append(jnp.concatenate(taps, axis=1))
        got = jnp.dot(
            turned_lines[k], jnp.concatenate(rows, axis=0), preferred_element_type=f32
        )
        for n in range(3):
            block = {0: n, 1: 3 * n + 2, 2: 6 + n, 3: 3 * n}[k]
            acc[:, block * C : (block + 1) * C] += got[:, n * C : (n + 1) * C]
    put_blocks(acc, out)


def mix_tile(fields, padded, wide, right, t, tile):
    widen(padded, t, wide)
    for first in range(0, S // 2, 8):
        for row, value in pair_conv(wide, t, first, 8, right[...]):
            tile[row] = (fields[t, row].astype(f32) + value).astype(bf16)


def make_mixed_body(t):
    def body(fields, padded, right, tile, wide):
        mix_tile(fields, padded, wide, right, t, tile)

    return body


def last_mixed_body(fields, padded, right, first, second, third, out, tile, sems, wide):
    copies = [
        pltpu.make_async_copy(source, out.at[t], sems.at[t])
        for t, source in enumerate((first, second, third, tile))
    ]
    for copy in copies[:3]:
        copy.start()
    mix_tile(fields, padded, wide, right, 3, tile)
    copies[3].start()
    for copy in copies:
        copy.wait()


def move(x=0, y=0, z=0):
    return 1 | (y << 1) | ((z >> 1) << 3) | (x << 5) | ((z & 1) << 7)


def parity(value):
    return bin(value).count("1") & 1


def dual(basis):
    size = len(basis)
    rows = [[(m >> k) & 1 for k in range(size)] + [int(k == i) for k in range(size)] for i, m in enumerate(basis)]
    for c in range(size):
        pivot = next(r for r in range(c, size) if rows[r][c])
        rows[c], rows[pivot] = rows[pivot], rows[c]
        for r in range(size):
            if r != c and rows[r][c]:
                rows[r] = [p ^ q for p, q in zip(rows[r], rows[c])]
    return [sum(rows[k][size + i] << k for k in range(size)) for i in range(size)]


CORE = 1
ALONG_X = [move(x=1), move(x=3)]
ALONG_Y = [move(y=1), move(y=3)]
ALONG_Z = [move(z=1), move(z=2), move(z=7)]
MOVES = ([CORE] + ALONG_X + ALONG_Y + ALONG_Z, [CORE] + ALONG_Y + ALONG_X + ALONG_Z)
DUALS = tuple(dual(m) for m in MOVES)


def place_bits(index):
    def bit(mask):
        v = index & mask
        v = v ^ (v >> 4)
        v = v ^ (v >> 2)
        return ((v ^ (v >> 1)) & 1) == 1

    half = bit(DUALS[0][0])
    bits = [half]
    for i in range(1, 5):
        bits.append(jnp.where(half, bit(DUALS[1][i]), bit(DUALS[0][i])))
    return bits


def exchange(value, ids):
    pairs = []
    for index in range(256):
        half = parity(index & DUALS[0][0])
        target = index
        for i in ids:
            target ^= MOVES[half][i]
        pairs.append((index, target))
    return lax.ppermute(value, MESH, pairs)


def pick(chunks, bits, flips):
    if not bits:
        return chunks[0]
    half = len(chunks) // 2
    low = pick(chunks[:half], bits[1:], flips[1:])
    high = pick(chunks[half:], bits[1:], flips[1:])
    return jnp.where(bits[0], low, high) if flips[0] else jnp.where(bits[0], high, low)


SUBSETS = {1: [(1,)], 2: [(1, 1), (0, 1), (1, 0)]}


def named(ids, flips):
    return tuple(i for i, f in zip(ids, flips) if f)


def scatter(value, ids, bits):
    parts = 1 << len(ids)
    rows = value.shape[0] // parts
    chunks = [value[i * rows : (i + 1) * rows] for i in range(parts)]
    mine = [bits[i] for i in ids]
    got = [
        exchange(pick(chunks, mine, flips).astype(bf16), named(ids, flips))
        for flips in SUBSETS[len(ids)]
    ]
    out = pick(chunks, mine, (0,) * len(ids))
    for part in got:
        out = out + part.astype(f32)
    return out


def spread(value, ids, bits):
    if len(ids) == 1:
        return value + exchange(value, ids)
    a, b = ids
    both, second, first = exchange(value, ids), exchange(value, (b,)), exchange(value, (a,))
    return (value + first) + (second + both)


def gather(value, ids, bits):
    got = {(0,) * len(ids): value}
    for flips in SUBSETS[len(ids)]:
        got[flips] = exchange(value, named(ids, flips))
    mine = [bits[i] for i in ids]
    parts = [got[key] for key in sorted(got)]
    return jnp.concatenate([pick(parts, mine, key) for key in sorted(got)])


def sum_everywhere(first, second, scale, bits, pieces):
    half = bits[0]
    value = jnp.where(half, second, first) + exchange(jnp.where(half, first, second), (0,))
    tiles = []
    for step, ids in ((scatter, (1, 2)), (scatter, (3, 4)), (spread, (5, 6)), (spread, (7,))):
        value = step(value, ids, bits)
        value, tile = lax.optimization_barrier((value, pieces(tiles)))
        tiles.append(tile)
    value = (value * scale).astype(bf16)
    value = gather(value, (3, 4), bits)
    value = gather(value, (1, 2), bits).reshape(3, 3, C, C)
    other = exchange(value, (0,))
    return (
        jnp.where(half, other, value).astype(f32),
        jnp.where(half, value, other).astype(f32),
        tiles[-1],
    )


def local(fields, cotangent, w_first, w_second, tile_links):
    count = lax.axis_size("space")
    own = lax.axis_index("space").astype(jnp.int32)
    bits = place_bits(lax.axis_index("dp").astype(jnp.int32) * count + own)
    own, *bits = lax.optimization_barrier((own, *bits))
    own = own.reshape(1)
    partner = [(i, i ^ 1) for i in range(count)]
    neighbour = [(i, (i + 1 if i % 2 else i - 1) % count) for i in range(count)]
    table, near, far, rim, x, cot, w_second, w_first, cot_lines = call(
        make_edges_body(count),
        [
            shape((36, 2), jnp.int32),
            shape((T, SEND, C), bf16),
            shape((T, SEND, C), bf16),
            shape((16 * RIM, C), f32),
            shape((T, S, S, C), bf16),
            shape((T, S, S, C), bf16),
            shape((3, 3, C, C), bf16),
            shape((3, 3, C, C), bf16),
            shape((4, T * S, C), f32),
        ],
        "shhhhh",
        [
            pltpu.VMEM((16 * S, C), f32),
            pltpu.VMEM((16 * 64, C), f32),
            pltpu.VMEM((16 * S, C), f32),
            pltpu.SMEM((T, 4, 5), jnp.int32),
            pltpu.SemaphoreType.DMA((5,)),
        ],
        outs_in="svvvvvvvv",
    )(
        own,
        *[
            pltpu.with_memory_space_constraint(v, pltpu.HBM)
            for v in (
                tile_links,
                fields.reshape(T, S, S, C),
                cotangent.reshape(T, S, S, C),
                w_second,
                w_first,
            )
        ],
    )
    from_far = lax.ppermute(far, "space", neighbour)
    from_near = lax.ppermute(near, "space", partner)
    interior, padded_x, first_right = call(
        conv_back_body,
        [shape((T, PIX, C), f32), shape((T, PAD, C), f32), shape((12 * C, 2 * C), bf16)],
        "vvvv",
        [
            pltpu.VMEM((T, PAD, C), f32),
            pltpu.VMEM((T, WIDE, 3 * C), bf16),
            pltpu.VMEM((12 * C, 2 * C), bf16),
        ],
    )(cot, w_second, x, w_first)
    active, hidden_grad, wide, act_near, act_far, *_ = call(
        forward_body,
        [
            shape((T, S, S, C), bf16),
            shape((T, PIX, C), bf16),
            shape((T, WIDE, 3 * C), bf16),
            shape((T, S, C), bf16),
            shape((T, S, C), bf16),
            shape((T, PAD, C), f32),
            shape((T, PIX, C), f32),
        ],
        "svvvvvv",
        [
            pltpu.VMEM((24 * S, C), f32),
            pltpu.VMEM((24 * RIM, C), f32),
            pltpu.VMEM((T, PIX, C), f32),
            pltpu.VMEM((T, 4 * S, C), f32),
        ],
        aliases={1: 5, 5: 6},
    )(table, padded_x, from_near, from_far, rim, interior, first_right)
    act_from_far = lax.ppermute(act_far, "space", neighbour)
    act_from_near = lax.ppermute(act_near, "space", partner)
    grad_first, padded_active, inner, turned_lines, second_right = call(
        first_grad_body,
        [
            shape((9 * C, C), f32),
            shape((T, PAD, C), f32),
            shape((C, 9 * C), f32),
            shape((4, C, T * S), bf16),
            shape((12 * C, 2 * C), bf16),
        ],
        "vvvvvv",
        [pltpu.VMEM((C, 9 * C), f32), pltpu.VMEM((T, WIDE, 3 * C), bf16)],
    )(hidden_grad, wide, active, cot, w_second, cot_lines)
    grad_second, padded_active = call(
        second_grad_body,
        [shape((9 * C, C), f32), shape((T, PAD, C), f32)],
        "svvvvv",
        [pltpu.VMEM((24 * S, C), f32), pltpu.VMEM((C, 9 * C), f32)],
        aliases={1: 1},
    )(table, padded_active, act_from_near, act_from_far, inner, turned_lines)

    def mixed_piece(tiles):
        t = len(tiles)
        if t < T - 1:
            (tile,) = call(
                make_mixed_body(t),
                [shape((S, S, C), bf16)],
                "vvv",
                [pltpu.VMEM((T, WIDE, 3 * C), bf16)],
            )(x, padded_active, second_right)
            return tile
        (mixed,) = call(
            last_mixed_body,
            [shape((T, S, S, C), bf16)],
            "vvvvvv",
            [
                pltpu.VMEM((S, S, C), bf16),
                pltpu.SemaphoreType.DMA((T,)),
                pltpu.VMEM((T, WIDE, 3 * C), bf16),
            ],
            outs_in="h",
        )(x, padded_active, second_right, *tiles)
        return mixed

    total = lax.axis_size("dp") * count * T * PIX
    first, second, mixed = sum_everywhere(
        grad_first, grad_second, float(total) ** -0.5, bits, mixed_piece
    )
    return (
        mixed.reshape(fields.shape),
        first,
        second,
    )


def solution(mesh):
    placed = (
        P("dp", "space", None, None, None),
        P("dp", "space", None, None, None),
        P(),
        P(),
        P("space", None, None),
    )
    return jax.shard_map(
        local,
        mesh=mesh,
        in_specs=placed,
        out_specs=(P("dp", "space", None, None, None), P(), P()),
        check_vma=False,
    )
```
